32 devices in a mesh: node: 8 (over z, y), feat: 4 (over x, core).
Axes of the slice: x: 2, y: 2, z: 4, core: 2. Of those that a mesh axis runs over, the one named last changes fastest.
Arguments:
- memory: float32 [8192, 172], P('node')
- last_update: int32 [8192], P('node'), may hold values from 6000 to 9999
- ev_time: int32 [16384], P(('node', 'feat')), may hold values from 10000 to 11999
- nbr_gap: int32 [16384, 10], P(('node', 'feat')), may hold values from 1 to 1999
- slot_rows: int32 [32, 1536], P(('node', 'feat')), may hold values from -1 to 1023, as said below
- slot_ref: int32 [16384, 12], P(('node', 'feat')), may hold values from 0 to 1535, as said below
- edge_feat: bfloat16 [16384, 256], P('node', 'feat'), may hold values from -6 to 6
- frequency: float32 [100], replicated, may hold values from 0.001 to 0.1
- phase_shift: float32 [100], replicated, may hold values from -3.140625 to 3.140625
- w_query: bfloat16 [272, 272], replicated, may hold values from -0.375 to 0.375
- w_key: bfloat16 [272, 272], replicated, may hold values from -0.375 to 0.375
- w_value: bfloat16 [272, 272], replicated, may hold values from -0.375 to 0.375
- w_merge: bfloat16 [444, 172], replicated, may hold values from -0.25 to 0.25
- b_merge: float32 [172], replicated, may hold values from -3 to 3
- w_out: bfloat16 [172, 172], replicated, may hold values from -0.4375 to 0.4375
- b_out: float32 [172], replicated, may hold values from -3 to 3
- w_input: float32 [3, 700, 172], P(None, None, 'feat'), may hold values from -0.21875 to 0.21875
- w_hidden: float32 [3, 172, 172], P(None, None, 'feat'), may hold values from -0.4375 to 0.4375
- gru_bias: float32 [4, 172], P(None, 'feat'), may hold values from -3 to 3
Outputs:
- embedding: bfloat16 [16384, 172], P(('node', 'feat'))
- new_memory: float32 [8192, 172], P('node', 'feat')
The draws below stay inside these ranges and needn't reach their ends.
Inputs may be any that keep to these rules, and one draw needn't show every extreme that they name: `slot_rows`: row r lists the nodes read by events r * 512 to (r + 1) * 512 - 1: slot s asks owner s // 192 (an index along node) for one of its local rows, or holds -1. Within one owner's 192 slots the live ones come first and name distinct rows; every row has 1024 live slots. `slot_ref`: entries of event e name live slots of row e // 512 of slot_rows; every live slot is named by some event of its block.
All inputs are finite; a program needn't handle non-finite values.
Results may differ from the reference program's by a relative error of at most 0.01.
Values may be sent and summed in bfloat16 or wider, within the bound.
No kernel may reach another device: no remote copies, remote signals or barrier semaphores. Data moves between devices by JAX's collectives and lax.ppermute only.
A program may use at most 128 MiB of HBM per device.

```python
import math
import jax
import jax.numpy as jnp
from jax import lax

MEM = 172
TIME = 100
MSGF = 256
EMB = 172
HEADS = 2
K = 10
EV_DEV = 512
NODE_DEV = 1024
ATT = 272
RAW = 700
CAP = 192
SLOTS = 1536
NODES = 8192
EVENTS = 16384
N_NODE = 8
N_FEAT = 4


def layout(key):
    device_total = N_NODE * N_FEAT
    quarter = EV_DEV // N_NODE
    key_hot, key_low, key_rows, key_first, key_extra, key_mix = jax.random.split(key, 6)
    hottest = jax.random.randint(key_hot, (), 0, N_NODE)
    lightest = (hottest + jax.random.randint(key_low, (device_total,), 1, N_NODE)) % N_NODE
    owners = jnp.arange(N_NODE, dtype=jnp.int32)
    loads = jnp.where(owners[None, :] == hottest, 3 * quarter, jnp.where(owners[None, :] == lightest[:, None], quarter, 2 * quarter))
    row_keys = jax.random.split(key_rows, device_total * N_NODE)
    drawn_rows = jax.vmap(lambda subkey: jax.random.permutation(subkey, NODE_DEV)[:CAP])(row_keys)
    drawn_rows = drawn_rows.reshape(device_total, N_NODE, CAP).astype(jnp.int32)
    filled = jnp.arange(CAP, dtype=jnp.int32)[None, None, :] < loads[:, :, None]
    slot_rows = jnp.where(filled, drawn_rows, -1).reshape(device_total, SLOTS).astype(jnp.int32)
    ranking = (1 - filled.reshape(device_total, SLOTS).astype(jnp.int32)) * SLOTS + jnp.arange(SLOTS, dtype=jnp.int32)[None, :]
    live_slots = jnp.argsort(ranking, axis=1)[:, :2 * EV_DEV].astype(jnp.int32)
    entry_total = EV_DEV * (K + 2)
    covering = jax.vmap(lambda subkey: jax.random.permutation(subkey, 2 * EV_DEV))(jax.random.split(key_first, device_total))
    further = jax.random.randint(key_extra, (device_total, entry_total - 2 * EV_DEV), 0, 2 * EV_DEV)
    picks = jnp.concatenate([covering.astype(jnp.int32), further.astype(jnp.int32)], 1)
    picks = jax.vmap(lambda subkey, entries: jax.random.permutation(subkey, entries))(jax.random.split(key_mix, device_total), picks)
    slot_ref = jnp.take_along_axis(live_slots, picks, axis=1).reshape(device_total * EV_DEV, K + 2).astype(jnp.int32)
    return (slot_rows, slot_ref)


def draw_slot_rows(key, part):
    return layout(jax.random.fold_in(key, 3))[0]


def draw_slot_ref(key, part):
    return layout(jax.random.fold_in(key, 3))[1]


def draw_memory(key, part):
    key = jax.random.fold_in(key, 11)
    key_base = jax.random.fold_in(key, 0)
    base_vals = jnp.clip(jax.random.normal(key_base, (NODES, MEM), jnp.float32), -6.0, 6.0)
    return base_vals


def set_ends(values, own_key, low, top_value):
    place = [jax.random.randint(jax.random.fold_in(own_key, axis), (), 0, length) for axis, length in enumerate(values.shape)]
    widest = values.shape.index(max(values.shape))
    beside = place[:widest] + [(place[widest] + 1) % values.shape[widest]] + place[widest + 1:]
    return values.at[tuple(place)].set(low).at[tuple(beside)].set(top_value)


def block_levels(rng, extent, cuts, least, high):
    loudness, own = 1.0, jax.random.fold_in(rng, 6)
    for axis_at, parts in cuts:
        draws = jnp.exp(jax.random.uniform(jax.random.fold_in(own, axis_at), (parts,), jnp.float32, least / len(cuts), high / len(cuts)))
        loudness = loudness * jnp.repeat(draws, extent[axis_at] // parts).reshape([-1 if axis == axis_at else 1 for axis in range(len(extent))])
    return loudness


def noise(key, dims, scale, bound, cuts=(), kind=jnp.bfloat16):
    drawn = jax.random.normal(key, dims, jnp.float32) * scale
    if len(cuts) > 0:
        drawn = block_levels(key, dims, cuts, -0.22, 0.18) * drawn
    return jnp.clip(drawn, min=-bound, max=bound).astype(kind)


def setup_inputs(seed: int = 0) -> dict:
    arg_keys = jax.random.split(jax.random.key(seed), 20)
    memory = draw_memory(jax.random.fold_in(arg_keys[19], 71), 0)
    last_update = set_ends(jax.random.randint(arg_keys[1], (NODES,), 6000, 10000), jax.random.fold_in(arg_keys[1], 1), 6000, 9999).astype(jnp.int32)
    ev_time = set_ends(jax.random.randint(arg_keys[2], (EVENTS,), 10000, 12000), jax.random.fold_in(arg_keys[2], 1), 10000, 11999).astype(jnp.int32)
    nbr_gap = set_ends(jax.random.randint(arg_keys[3], (EVENTS, K), 1, 2000), jax.random.fold_in(arg_keys[3], 1), 1, 1999).astype(jnp.int32)
    slot_rows = draw_slot_rows(jax.random.fold_in(arg_keys[19], 71), 0)
    slot_ref = draw_slot_ref(jax.random.fold_in(arg_keys[19], 71), 0)
    edge_feat = noise(arg_keys[6], (EVENTS, MSGF), 1.0, 6.0, ((0, 8), (1, 4)))
    frequency = jnp.clip(jnp.exp(jax.random.uniform(arg_keys[7], (TIME,), jnp.float32, math.log(0.001), math.log(0.1))), 0.001, 0.1)
    phase_shift = jnp.clip(jax.random.uniform(arg_keys[8], (TIME,), jnp.float32, -3.140625, 3.140625), -3.140625, 3.140625)
    w_query = noise(arg_keys[9], (ATT, ATT), ATT ** -0.5, 0.375)
    w_key = noise(arg_keys[10], (ATT, ATT), ATT ** -0.5, 0.375)
    w_value = noise(arg_keys[11], (ATT, ATT), ATT ** -0.5, 0.375)
    w_merge = noise(arg_keys[12], (ATT + MEM, EMB), (ATT + MEM) ** -0.5, 0.25)
    b_merge = noise(arg_keys[13], (EMB,), 0.5, 3.0, (), jnp.float32)
    w_out = noise(arg_keys[14], (EMB, EMB), EMB ** -0.5, 0.4375)
    b_out = noise(arg_keys[15], (EMB,), 0.5, 3.0, (), jnp.float32)
    w_input = noise(arg_keys[16], (3, RAW, MEM), RAW ** -0.5, 0.21875, ((2, 4),), jnp.float32)
    w_hidden = noise(arg_keys[17], (3, MEM, MEM), MEM ** -0.5, 0.4375, ((2, 4),), jnp.float32)
    gru_bias = noise(arg_keys[18], (4, MEM), 0.5, 3.0, ((1, 4),), jnp.float32)
    return dict(memory=memory, last_update=last_update, ev_time=ev_time, nbr_gap=nbr_gap, slot_rows=slot_rows, slot_ref=slot_ref, edge_feat=edge_feat, frequency=frequency, phase_shift=phase_shift, w_query=w_query, w_key=w_key, w_value=w_value, w_merge=w_merge, b_merge=b_merge, w_out=w_out, b_out=b_out, w_input=w_input, w_hidden=w_hidden, gru_bias=gru_bias)


precise = lax.Precision.HIGHEST

def time_code(gap_vals, frequency, phase_shift):
    return jnp.cos(gap_vals[..., None] * frequency + phase_shift)

def embed_events(source, neighbors, gap_vals, frequency, phase_shift, w_query, w_key, w_value, w_merge, b_merge, w_out, b_out):
    event_count = source.shape[0]
    nbr_count = neighbors.shape[1]
    att_width = w_query.shape[0]
    head_size = att_width // HEADS
    still_code = jnp.broadcast_to(jnp.cos(phase_shift), (event_count, phase_shift.shape[0]))
    query_in = jnp.concatenate([source, still_code], 1).astype(jnp.bfloat16)
    key_in = jnp.concatenate([neighbors, time_code(gap_vals, frequency, phase_shift)], 2).astype(jnp.bfloat16)
    key_in = key_in.reshape(event_count * nbr_count, att_width)
    queries = jnp.dot(query_in, w_query, preferred_element_type=jnp.float32).reshape(event_count, HEADS, head_size)
    key_vecs = jnp.dot(key_in, w_key, preferred_element_type=jnp.float32).reshape(event_count, nbr_count, HEADS, head_size)
    values = jnp.dot(key_in, w_value, preferred_element_type=jnp.float32).reshape(event_count, nbr_count, HEADS, head_size)
    scores = jnp.einsum('ehd,ekhd->ehk', queries, key_vecs, precision=precise) / math.sqrt(head_size)
    weights = jax.nn.softmax(scores, axis=2)
    attended = jnp.einsum('ehk,ekhd->ehd', weights, values, precision=precise).reshape(event_count, att_width)
    merged = jnp.concatenate([attended, source], 1).astype(jnp.bfloat16)
    hidden = jax.nn.relu(jnp.dot(merged, w_merge, preferred_element_type=jnp.float32) + b_merge).astype(jnp.bfloat16)
    return (jnp.dot(hidden, w_out, preferred_element_type=jnp.float32) + b_out).astype(jnp.bfloat16)

def build_messages(source, target, stamp_src, stamp_dst, ev_time, edge_rows, frequency, phase_shift):
    code_src = time_code((ev_time - stamp_src).astype(jnp.float32), frequency, phase_shift)
    code_dst = time_code((ev_time - stamp_dst).astype(jnp.float32), frequency, phase_shift)
    wide_edges = edge_rows.astype(jnp.float32)
    to_source = jnp.concatenate([source, target, code_src, wide_edges], 1)
    to_target = jnp.concatenate([target, source, code_dst, wide_edges], 1)
    return jnp.concatenate([to_source, to_target], 0)

def gru_update(inputs, previous, own_cols, w_hidden, gru_bias):
    recurrent = jnp.einsum('rn,gnm->grm', previous, w_hidden, precision=precise)
    reset_gate = jax.nn.sigmoid(inputs[0] + recurrent[0] + gru_bias[0])
    update_gate = jax.nn.sigmoid(inputs[1] + recurrent[1] + gru_bias[1])
    candidate = jnp.tanh(inputs[2] + gru_bias[2] + reset_gate * (recurrent[2] + gru_bias[3]))
    return (1.0 - update_gate) * candidate + update_gate * own_cols

def reference(memory, last_update, ev_time, nbr_gap, slot_rows, slot_ref, edge_feat, frequency, phase_shift, w_query, w_key, w_value, w_merge, b_merge, w_out, b_out, w_input, w_hidden, gru_bias):
    block_total = EVENTS // EV_DEV
    owner_of = (slot_ref // CAP).astype(jnp.int32)
    block_of = (jnp.arange(EVENTS, dtype=jnp.int32) // EV_DEV).astype(jnp.int32)
    local_rows = slot_rows[block_of[:, None], slot_ref]
    node_ids = (owner_of * NODE_DEV + local_rows).astype(jnp.int32)

    def scan_block(state_pair, block_inputs):
        totals, hit_counts = state_pair
        block_ids, block_times, block_gaps, edge_rows = block_inputs
        fetched = memory[block_ids]
        stamps = last_update[block_ids[:, :2]]
        embedded = embed_events(fetched[:, 0], fetched[:, 2:], block_gaps.astype(jnp.float32), frequency, phase_shift, w_query, w_key, w_value, w_merge, b_merge, w_out, b_out)
        message_rows = build_messages(fetched[:, 0], fetched[:, 1], stamps[:, 0], stamps[:, 1], block_times, edge_rows, frequency, phase_shift)
        endpoints = jnp.concatenate([block_ids[:, 0], block_ids[:, 1]])
        totals = totals.at[endpoints].add(message_rows)
        hit_counts = hit_counts.at[endpoints].add(jnp.ones(endpoints.shape, jnp.float32))
        return ((totals, hit_counts), embedded)
    initial = (jnp.zeros((NODES, RAW), jnp.float32), jnp.zeros((NODES,), jnp.float32))
    scanned = (node_ids.reshape(block_total, EV_DEV, K + 2), ev_time.reshape(block_total, EV_DEV), nbr_gap.reshape(block_total, EV_DEV, K), edge_feat.reshape(block_total, EV_DEV, MSGF))
    (totals, hit_counts), embedded = lax.scan(scan_block, initial, scanned)
    averaged = totals / jnp.maximum(hit_counts, 1.0)[:, None]
    inputs = jnp.einsum('rn,gnm->grm', averaged, w_input, precision=precise)
    renewed = gru_update(inputs, memory, memory, w_hidden, gru_bias)
    new_memory = jnp.where((hit_counts > 0.0)[:, None], renewed, memory)
    return (embedded.reshape(EVENTS, EMB), new_memory)
```

```python
import functools
import math

import jax
import jax.numpy as jnp
from jax import lax
from jax.experimental import pallas as pl
from jax.experimental.pallas import tpu as pltpu
from jax.sharding import PartitionSpec as P

HEADS = 2
LANES = 128
HALF = 64
GROUP = 8
EVENT_TILE = 128
STAMP_SHIFT = 6
HIT_BASE = 32.0

bf16 = jnp.bfloat16
f32 = jnp.float32
exact = lax.Precision.HIGHEST


def rounded(count, step):
    return -(-count // step) * step


def cosine(x):
    turns = jnp.floor(x * (1.0 / math.pi) + 0.5)
    r = x - turns * 3.140625
    r = r - turns * 9.67502593994140625e-4
    r = r - turns * 1.509957990978376432e-7
    half = turns * 0.5
    sign = 1.0 - 4.0 * (half - jnp.floor(half))
    s = r * r
    poly = 1.0 / 479001600.0
    for coef in (-1.0 / 3628800.0, 1.0 / 40320.0, -1.0 / 720.0, 1.0 / 24.0, -0.5, 1.0):
        poly = poly * s + coef
    return poly * sign


def mm(a, b):
    return jnp.dot(a, b, preferred_element_type=f32)


def mm_nt(a, b):
    return lax.dot_general(a, b, (((1,), (1,)), ((), ())), preferred_element_type=f32)


def hot(mask):
    return jnp.where(mask, 1.0, 0.0).astype(bf16)


def iota(shape, axis):
    return lax.broadcasted_iota(jnp.int32, shape, axis)


PART, TIME_AT, EDGE_AT, COLS = 256, 256, 384, 640
PIECES = COLS // LANES
SPARE_ROWS = 16


def pack_kernel(mem, time, feat, feat_ref, edge_ref, w_ref, *out_refs):
    own, events = edge_ref.shape
    events = events // feat
    gates, width, raw = w_ref.shape
    lines = jnp.concatenate([w_ref[g] for g in range(gates)], 0)
    spare = gates * width - LANES
    lines = jnp.concatenate([lines, jnp.zeros((LANES + SPARE_ROWS - gates * width, raw), f32)], 0)
    height = lines.shape[0]
    fill = lambda count: jnp.zeros((height, count), f32)
    lines = jnp.concatenate(
        [
            lines[:, mem : 2 * mem],
            fill(PART - mem),
            lines[:, 2 * mem : 2 * mem + time],
            fill(LANES - time),
            lines[:, 2 * mem + time :],
        ],
        1,
    ).astype(bf16)
    edge_rows = own * events // LANES
    for k, out_ref in enumerate(out_refs):
        dest = lax.rem(feat_ref[0] + k, feat)
        block = edge_ref[:, pl.ds(pl.multiple_of(dest * events, LANES), events)]
        for c in range(events // LANES):
            out_ref[c * own : (c + 1) * own, :] = block[:, c * LANES : (c + 1) * LANES]
        for c in range(PIECES):
            at = edge_rows + c * height
            out_ref[at : at + height, :] = lines[:, c * LANES : (c + 1) * LANES]


def rows_kernel(feat, feat_ref, ids_ref, memory_ref, stamp_ref, out_ref):
    nodes, _, _ = out_ref.shape
    per_owner = ids_ref.shape[1]
    mem, rows = memory_ref.shape
    stamps = stamp_ref[...]
    high = lax.shift_right_logical(stamps, STAMP_SHIFT)
    low = stamps - lax.shift_left(high, STAMP_SHIFT)
    tail = jnp.concatenate([high, low, jnp.zeros((2 * LANES - mem - 2, rows), jnp.int32)], 0).astype(f32)
    table = jnp.concatenate([memory_ref[...], tail], 0).astype(bf16)
    wanted = jnp.concatenate([ids_ref[pl.ds(n * feat + feat_ref[0], 1), :] for n in range(nodes)], 0)
    columns = jnp.transpose(wanted)
    for n in range(nodes):
        picked = mm_nt(hot(columns[:, n : n + 1] == iota((per_owner, rows), 1)), table)
        out_ref[n, 0:per_owner, :] = picked[:, :LANES].astype(bf16)
        tail = picked[:, LANES : LANES + HALF]
        tail = jnp.concatenate([tail[: per_owner // 2], tail[per_owner // 2 :]], 1)
        room = out_ref.shape[1] - per_owner - per_owner // 2
        if room:
            tail = jnp.concatenate([tail, jnp.zeros((room, LANES), f32)], 0)
        out_ref[n, per_owner:, :] = tail.astype(bf16)


def message_kernel(mem, per_owner, feat, own, feat_ref, rows_ref, ref_ref, reft_ref, time_ref, freq_ref, phase_ref, *rest):
    pack_refs = rest[:feat]
    table_ref, out_ref, w_ref, x_ref, edge_ref = rest[feat:]
    nodes = rows_ref.shape[0]
    slots = nodes * per_owner
    events = ref_ref.shape[0]
    time = freq_ref.shape[1]
    source_of = [lax.rem(feat_ref[0] + feat - k, feat) for k in range(feat)]
    for n in range(nodes):
        at = n * per_owner
        table_ref[at : at + per_owner, 0:LANES] = rows_ref[n, 0:per_owner, :]
        tail = rows_ref[n, per_owner : per_owner + per_owner // 2, :].astype(f32)
        tail = jnp.concatenate([tail[:, :HALF], tail[:, HALF:]], 0)
        tail = jnp.concatenate([tail, jnp.zeros((per_owner, HALF), f32)], 1)
        table_ref[at : at + per_owner, LANES : 2 * LANES] = tail.astype(bf16)
    edge_rows = own * events // LANES
    height = LANES + SPARE_ROWS
    spare = []
    for k in range(feat):
        for c in range(PIECES):
            at = edge_rows + c * height
            w_ref[k * LANES : (k + 1) * LANES, c * LANES : (c + 1) * LANES] = pack_refs[k][at : at + LANES, :]
        spare.append(
            jnp.concatenate(
                [
                    pack_refs[k][edge_rows + c * height + LANES : edge_rows + (c + 1) * height, :].astype(f32)[0:1]
                    for c in range(PIECES)
                ],
                1,
            )
        )
        for c in range(events // LANES):
            edge_ref[pl.ds(pl.multiple_of(source_of[k] * own, own), own), c * LANES : (c + 1) * LANES] = pack_refs[k][
                c * own : (c + 1) * own, :
            ]
    spare = jnp.concatenate(spare + [jnp.zeros((SPARE_ROWS - feat, COLS), f32)], 0).astype(bf16)
    edges = edge_ref[...]
    table = table_ref[...]
    slot_of = iota((events, slots), 1)
    hot_src = hot(ref_ref[:, 0:1] == slot_of)
    hot_dst = hot(ref_ref[:, 1:2] == slot_of)
    source = mm(hot_src, table)
    target = mm(hot_dst, table)
    freq = freq_ref[...]
    phase = phase_ref[...]

    def code(rows):
        stamps = rows[:, mem : mem + 1] * float(1 << STAMP_SHIFT) + rows[:, mem + 1 : mem + 2]
        return cosine((time_ref[...].astype(f32) - stamps) * freq + phase).astype(bf16)

    code_src = code(source)
    code_dst = code(target)
    source = source.astype(bf16)
    target = target.astype(bf16)
    w_part = w_ref[:, 0:PART]
    w_time = w_ref[:, TIME_AT : TIME_AT + time]
    by_edge = lax.dot_general(edges, w_ref[:, EDGE_AT:COLS], (((0,), (1,)), ((), ())), preferred_element_type=f32)
    to_src = (mm_nt(target, w_part) + mm_nt(code_src, w_time) + by_edge).astype(bf16)
    to_dst = (mm_nt(source, w_part) + mm_nt(code_dst, w_time) + by_edge).astype(bf16)
    s_part, s_time, s_edge = spare[:, :PART], spare[:, TIME_AT : TIME_AT + time], spare[:, EDGE_AT:]
    line_edge = mm(s_edge, edges)
    ones = iota((SPARE_ROWS, events), 0) == feat
    line_src = jnp.where(ones, 1.0, mm_nt(s_part, target) + mm_nt(s_time, code_src) + line_edge).astype(bf16)
    line_dst = jnp.where(ones, 1.0, mm_nt(s_part, source) + mm_nt(s_time, code_dst) + line_edge).astype(bf16)
    lines = mm(line_src, hot_src) + mm(line_dst, hot_dst)
    x_ref[:, 0:slots] = lines[0:8]
    back_src = hot(iota((slots, events), 0) == reft_ref[0:1, :])
    back_dst = hot(iota((slots, events), 0) == reft_ref[1:2, :])
    sums = (mm(back_src, to_src) + mm(back_dst, to_dst)).astype(bf16)
    groups = -(-per_owner // LANES)
    row_id = iota((GROUP, LANES), 0)
    extra = out_ref.shape[1] - per_owner
    for n in range(nodes):
        at = n * per_owner
        blocks = []
        for c in range(groups):
            x = x_ref[:, at + c * LANES : at + (c + 1) * LANES]
            hits = x[feat : feat + 1, :]
            high = jnp.floor(hits * (1.0 / HIT_BASE))
            low = hits - high * HIT_BASE
            blocks.append((x, high, low))
        for k in range(feat):
            tail = [
                jnp.where(row_id == 0, x[k : k + 1, :], jnp.where(row_id == 1, high, jnp.where(row_id == 2, low, 0.0)))
                for x, high, low in blocks
            ]
            if extra > GROUP * groups:
                tail.append(jnp.zeros((extra - GROUP * groups, LANES), f32))
            dest = n * feat + source_of[k]
            out_ref[dest, 0:per_owner, :] = sums[at : at + per_owner, k * LANES : (k + 1) * LANES]
            out_ref[dest, per_owner:, :] = jnp.concatenate(tail, 0).astype(bf16)


def embed_kernel(mem, table_ref, ref_ref, gap_ref, freq_ref, phase_ref, wq_ref, wk_ref, wv_ref, wm_ref, bm_ref, wo_ref, bo_ref, out_ref, hot_ref, key_ref, prod_ref):
    tile, columns = ref_ref.shape
    nbrs = columns - 2
    slots = table_ref.shape[0]
    att = wq_ref.shape[0]
    head = att // HEADS
    slot_of = iota((tile, slots), 1)
    hot_ref[0:tile, :] = hot(ref_ref[:, 0:1] == slot_of)
    for k in range(nbrs):
        hot_ref[(k + 1) * tile : (k + 2) * tile, :] = hot(ref_ref[:, 2 + k : 3 + k] == slot_of)
    fetched = mm(hot_ref[...], table_ref[...])
    freq = freq_ref[...]
    phase = phase_ref[...]
    kept = iota((tile, LANES), 1) < mem - LANES
    for k in range(nbrs + 1):
        at = k * tile
        if k == 0:
            angle = jnp.broadcast_to(phase, (tile, 2 * LANES))
        else:
            angle = gap_ref[:, k - 1 : k].astype(f32) * freq + phase
        wave = cosine(angle)
        key_ref[at : at + tile, 0:LANES] = fetched[at : at + tile, :LANES].astype(bf16)
        key_ref[at : at + tile, LANES : 2 * LANES] = jnp.where(kept, fetched[at : at + tile, LANES:], wave[:, :LANES]).astype(bf16)
        key_ref[at : at + tile, 2 * LANES : att] = wave[:, LANES : att - LANES].astype(bf16)
    query = mm(key_ref[0:tile, :], wq_ref[...]) * (1.0 / math.sqrt(head))
    keys = mm(key_ref[tile:, :], wk_ref[...])
    values = mm(key_ref[tile:, :], wv_ref[...])
    for k in range(nbrs):
        prod_ref[k * tile : (k + 1) * tile, :] = keys[k * tile : (k + 1) * tile, :] * query
    prod = prod_ref[...]
    gather = hot((iota((att, LANES), 0) >= head).astype(jnp.int32) == (iota((att, LANES), 1) & 1))
    high = prod.astype(bf16)
    scores = mm(high, gather) + mm((prod - high.astype(f32)).astype(bf16), gather)
    parts = [scores[k * tile : (k + 1) * tile, :] for k in range(nbrs)]
    top = functools.reduce(jnp.maximum, parts)
    parts = [jnp.exp(s - top) for s in parts]
    scale = 1.0 / functools.reduce(jnp.add, parts)
    spread = hot(
        ((iota((LANES, att), 1) >= head).astype(jnp.int32) == (iota((LANES, att), 0) & 1)) & (iota((LANES, att), 0) < 4)
    )
    upper = iota((tile, LANES), 1) < 2
    attended = jnp.zeros((tile, att), f32)
    for k in range(nbrs):
        w = parts[k] * scale
        w_high = w.astype(bf16).astype(f32)
        w = jnp.where(upper, w_high, w - w_high).astype(bf16)
        attended = attended + mm(w, spread) * values[k * tile : (k + 1) * tile, :]
    merged = mm(attended.astype(bf16), wm_ref[0:att, :]) + mm(key_ref[0:tile, 0:mem], wm_ref[att : att + mem, :])
    hidden = jnp.maximum(merged + bm_ref[...], 0.0).astype(bf16)
    out_ref[...] = (mm(hidden, wo_ref[...]) + bo_ref[...]).astype(bf16)


def state_kernel(memory_ref, w_in_ref, w_hid_ref, bias_ref, out_ref):
    memory = memory_ref[...]
    mem = memory.shape[0]
    bias = bias_ref[...]

    def part(w, g):
        out_ref[g] = jnp.dot(w, memory, precision=exact, preferred_element_type=f32) + bias[:, g : g + 1]

    part(w_in_ref[0, :, 0:mem] + w_hid_ref[0], 0)
    part(w_in_ref[1, :, 0:mem] + w_hid_ref[1], 1)
    part(w_in_ref[2, :, 0:mem], 2)
    part(w_hid_ref[2], 3)


def update_kernel(per_owner, per_step, recv_ref, ids_ref, state_ref, own_ref, out_ref, acc_ref, turned_ref):
    rows = acc_ref.shape[0]
    width = own_ref.shape[0]
    groups = -(-per_owner // LANES)
    acc_ref[...] = jnp.zeros_like(acc_ref)

    def step(i, carry):
        main, side = [], []
        for b in range(per_step):
            block = i * per_step + b
            main.append(recv_ref[block, 0:per_owner, :])
            tail = recv_ref[block, per_owner:, :].astype(f32)
            for c in range(groups):
                count = min(LANES, per_owner - c * LANES)
                side.append(jnp.transpose(tail[c * GROUP : (c + 1) * GROUP, :])[:count, :])
        side = jnp.concatenate(side, 0)
        side = jnp.concatenate([side, jnp.zeros((side.shape[0], LANES - GROUP), f32)], 1).astype(bf16)
        data = jnp.concatenate([jnp.concatenate(main, 0), side], 1)
        ids = ids_ref[i]
        acc_ref[...] += mm(hot(iota((rows, ids.shape[1]), 0) == ids), data)
        return carry

    lax.fori_loop(0, recv_ref.shape[0] // per_step, step, 0)
    turned_ref[...] = jnp.transpose(acc_ref[...])
    at = 3 * width
    hits = turned_ref[at : at + 1, :] * HIT_BASE + turned_ref[at + 1 : at + 2, :]
    scale = 1.0 / jnp.maximum(hits, 1.0)
    own = own_ref[...]
    reset = jax.nn.sigmoid(turned_ref[0:width, :] * scale + state_ref[0])
    update = jax.nn.sigmoid(turned_ref[width : 2 * width, :] * scale + state_ref[1])
    fresh = jnp.tanh(turned_ref[2 * width : 3 * width, :] * scale + state_ref[2] + reset * state_ref[3])
    out_ref[...] = jnp.where(hits > 0.0, (1.0 - update) * fresh + update * own, own)


def cost(flops, moved):
    return pl.CostEstimate(flops=int(flops), transcendentals=0, bytes_accessed=int(moved))


def per_device(
    memory,
    last_update,
    ev_time,
    nbr_gap,
    slot_rows,
    slot_ref,
    edge_feat,
    frequency,
    phase_shift,
    w_query,
    w_key,
    w_value,
    w_merge,
    b_merge,
    w_out,
    b_out,
    w_input,
    w_hidden,
    gru_bias,
):
    nodes = lax.axis_size("node")
    feat = lax.axis_size("feat")
    blocks = nodes * feat
    rows, mem = memory.shape
    slots = slot_rows.shape[1]
    per_owner = slots // nodes
    events, columns = slot_ref.shape
    time = frequency.shape[0]
    att = w_query.shape[0]
    emb = w_out.shape[1]
    width = w_hidden.shape[2]
    everyone = ("node", "feat")

    asked = jnp.broadcast_to(slot_rows.reshape(nodes, 1, per_owner), (nodes, feat, per_owner)).reshape(blocks, 1, per_owner)
    asked = lax.all_to_all(asked, everyone, split_axis=0, concat_axis=0, tiled=True).reshape(blocks, per_owner)

    here = lax.axis_index("feat").astype(jnp.int32)
    here_line = here.reshape(1)
    memory_t = memory.T
    w_input_t = jnp.swapaxes(w_input, 1, 2)
    w_hidden_t = jnp.swapaxes(w_hidden, 1, 2)
    smem = pl.BlockSpec(memory_space=pltpu.SMEM)
    vmem = pl.BlockSpec(memory_space=pltpu.VMEM)

    own = edge_feat.shape[1]
    height = own * events // LANES + PIECES * (LANES + SPARE_ROWS)
    packed = pl.pallas_call(
        functools.partial(pack_kernel, mem, time, feat),
        in_specs=[smem, vmem, vmem],
        out_shape=[jax.ShapeDtypeStruct((height, LANES), bf16)] * feat,
        cost_estimate=cost(1e8, 1e6),
        name="pack",
    )(here_line, edge_feat.T, w_input_t)
    packed = [packed[0]] + [
        lax.ppermute(packed[k], "feat", [(i, (i + k) % feat) for i in range(feat)]) for k in range(1, feat)
    ]

    room = rounded(per_owner + per_owner // 2, 16)
    found = pl.pallas_call(
        functools.partial(rows_kernel, feat),
        out_shape=jax.ShapeDtypeStruct((nodes, room, LANES), bf16),
        in_specs=[smem, vmem, vmem, vmem],
        cost_estimate=cost(1e9, 2e6),
        name="rows",
    )(here_line, asked, memory_t, last_update.reshape(1, rows))
    found = lax.all_to_all(found, "node", split_axis=0, concat_axis=0, tiled=True)

    state = pl.pallas_call(
        state_kernel,
        out_shape=jax.ShapeDtypeStruct((4, width, rows), f32),
        cost_estimate=cost(3e9, 3e6),
        name="state",
    )(memory_t, w_input_t, w_hidden_t, gru_bias.T)

    freq_line = frequency.reshape(1, time)
    phase_line = phase_shift.reshape(1, time)
    groups = -(-per_owner // LANES)
    depth = per_owner + rounded(GROUP * groups, 16)
    fetched, sums = pl.pallas_call(
        functools.partial(message_kernel, mem, per_owner, feat, own),
        in_specs=[smem] + [vmem] * (6 + feat),
        out_shape=(
            jax.ShapeDtypeStruct((slots, 2 * LANES), bf16),
            jax.ShapeDtypeStruct((blocks, depth, LANES), bf16),
        ),
        scratch_shapes=[
            pltpu.VMEM((feat * LANES, COLS), bf16),
            pltpu.VMEM((8, rounded(slots, LANES) + LANES), f32),
            pltpu.VMEM((feat * own, events), bf16),
        ],
        cost_estimate=cost(4e9, 4e6),
        name="messages",
    )(here_line, found, slot_ref, slot_ref.T[:2], ev_time.reshape(events, 1), freq_line, phase_line, *packed)
    sums = lax.all_to_all(sums, everyone, split_axis=0, concat_axis=0, tiled=True)

    shift = mem - LANES
    spread = ((0, 0), (shift, 2 * LANES - shift - time))
    nbrs = columns - 2
    whole = lambda shape: pl.BlockSpec(shape, lambda i: (0,) * len(shape))
    embedding = pl.pallas_call(
        functools.partial(embed_kernel, mem),
        grid=(events // EVENT_TILE,),
        in_specs=[
            whole((slots, 2 * LANES)),
            pl.BlockSpec((EVENT_TILE, columns), lambda i: (i, 0)),
            pl.BlockSpec((EVENT_TILE, nbrs), lambda i: (i, 0)),
            whole((1, 2 * LANES)),
            whole((1, 2 * LANES)),
            whole((att, att)),
            whole((att, att)),
            whole((att, att)),
            whole((att + mem, emb)),
            whole((1, emb)),
            whole((emb, emb)),
            whole((1, emb)),
        ],
        out_specs=pl.BlockSpec((EVENT_TILE, emb), lambda i: (i, 0)),
        out_shape=jax.ShapeDtypeStruct((events, emb), bf16),
        scratch_shapes=[
            pltpu.VMEM(((nbrs + 1) * EVENT_TILE, slots), bf16),
            pltpu.VMEM(((nbrs + 1) * EVENT_TILE, att), bf16),
            pltpu.VMEM((nbrs * EVENT_TILE, att), f32),
        ],
        cost_estimate=cost(2e10, 4e6),
        name="embed",
    )(
        fetched,
        slot_ref,
        nbr_gap,
        jnp.pad(freq_line, spread),
        jnp.pad(phase_line, spread),
        w_query,
        w_key,
        w_value,
        w_merge,
        b_merge.reshape(1, emb),
        w_out,
        b_out.reshape(1, emb),
    )

    span = 768
    per_step = span // per_owner
    steps = blocks // per_step
    new_memory = pl.pallas_call(
        functools.partial(update_kernel, per_owner, per_step),
        out_shape=jax.ShapeDtypeStruct((width, rows), f32),
        scratch_shapes=[pltpu.VMEM((rows, 2 * LANES), f32), pltpu.VMEM((2 * LANES, rows), f32)],
        cost_estimate=cost(4e9, 4e6),
        name="update",
    )(
        sums,
        asked.reshape(steps, 1, per_step * per_owner),
        state,
        lax.dynamic_slice_in_dim(memory_t, here * width, width, 0),
    )
    return (embedding, new_memory.T)


def solution(mesh):
    return jax.shard_map(
        per_device,
        mesh=mesh,
        in_specs=(
            P("node", None),
            P("node"),
            P(("node", "feat")),
            P(("node", "feat"), None),
            P(("node", "feat"), None),
            P(("node", "feat"), None),
            P("node", "feat"),
            P(),
            P(),
            P(),
            P(),
            P(),
            P(),
            P(),
            P(),
            P(),
            P(None, None, "feat"),
            P(None, None, "feat"),
            P(None, "feat"),
        ),
        out_specs=(P(("node", "feat"), None), P("node", "feat")),
        check_vma=False,
    )
```

```python
import functools
import math

import jax
import jax.numpy as jnp
from jax import lax
from jax.experimental import pallas as pl
from jax.experimental.pallas import tpu as pltpu
from jax.sharding import PartitionSpec as P


HEADS = 2
LANES = 128
HALF = 64
GROUP = 3
EVENT_TILE = 128
STAMP_SHIFT = 6
HIT_BASE = 32.0
SPLIT = 2

bf16 = jnp.bfloat16
f32 = jnp.float32
exact = lax.Precision.HIGHEST


def rounded(count, step):
    return -(-count // step) * step


def cosine(x):
    turns = jnp.floor(x * (1.0 / math.pi) + 0.5)
    r = x - turns * 3.140625
    r = r - turns * 9.67502593994140625e-4
    r = r - turns * 1.509957990978376432e-7
    half = turns * 0.5
    sign = 1.0 - 4.0 * (half - jnp.floor(half))
    s = r * r
    poly = 1.0 / 479001600.0
    for coef in (-1.0 / 3628800.0, 1.0 / 40320.0, -1.0 / 720.0, 1.0 / 24.0, -0.5, 1.0):
        poly = poly * s + coef
    return poly * sign


def mm(a, b):
    return jnp.dot(a, b, preferred_element_type=f32)


def mm_nt(a, b):
    return lax.dot_general(a, b, (((1,), (1,)), ((), ())), preferred_element_type=f32)


def hot(mask):
    return jnp.where(mask, 1.0, 0.0).astype(bf16)


def iota(shape, axis):
    return lax.broadcasted_iota(jnp.int32, shape, axis)


PART, TIME_AT, EDGE_AT, COLS = 256, 256, 384, 640
PIECES = COLS // LANES
SPARE_ROWS = 16


def pack_kernel(mem, time, feat, feat_ref, edge_ref, w_ref, memory_ref, stamp_ref, table_ref, *out_refs):
    rows = memory_ref.shape[1]
    stamps = stamp_ref[...]
    high = lax.shift_right_logical(stamps, STAMP_SHIFT)
    low = stamps - lax.shift_left(high, STAMP_SHIFT)
    tail = jnp.concatenate([high, low, jnp.zeros((table_ref.shape[0] - mem - 2, rows), jnp.int32)], 0).astype(f32)
    table_ref[...] = jnp.concatenate([memory_ref[...], tail], 0).astype(bf16)
    own, events = edge_ref.shape
    events = events // feat
    gates, width, raw = w_ref.shape
    lines = jnp.concatenate([w_ref[g] for g in range(gates)], 0)
    lines = jnp.concatenate([lines, jnp.zeros((LANES + SPARE_ROWS - gates * width, raw), f32)], 0)
    height = lines.shape[0]
    fill = lambda count: jnp.zeros((height, count), f32)
    lines = jnp.concatenate(
        [
            lines[:, mem : 2 * mem],
            fill(PART - mem),
            lines[:, 2 * mem : 2 * mem + time],
            fill(LANES - time),
            lines[:, 2 * mem + time :],
        ],
        1,
    ).astype(bf16)
    edge_rows = own * events // LANES
    for k, out_ref in enumerate(out_refs):
        dest = lax.rem(feat_ref[0] + k, feat)
        block = edge_ref[:, pl.ds(pl.multiple_of(dest * events, LANES), events)]
        for c in range(events // LANES):
            out_ref[c * own : (c + 1) * own, :] = block[:, c * LANES : (c + 1) * LANES]
        for c in range(PIECES):
            at = edge_rows + c * height
            out_ref[at : at + height, :] = lines[:, c * LANES : (c + 1) * LANES]


def places_of(slot, nodes, per_owner):
    full = per_owner // LANES * LANES
    owner = jnp.zeros_like(slot)
    for n in range(1, nodes):
        owner = owner + (slot >= n * per_owner).astype(jnp.int32)
    within = slot - owner * per_owner
    piece = lax.shift_right_logical(within, 7)
    return jnp.where(
        within < full,
        (piece * nodes + owner) * LANES + within - piece * LANES,
        full * nodes + owner * HALF + within - full,
    )


def swapped(x):
    return pltpu.roll(x, HALF, 1)


def left(shape):
    return iota(shape, 1) < HALF


def split_pair(tile):
    top, low = tile[: tile.shape[0] // 2], tile[tile.shape[0] // 2 :]
    side = left(top.shape)
    return jnp.where(side, top, swapped(low)), jnp.where(side, swapped(top), low)


def join_pair(first, second):
    side = left(first.shape)
    return jnp.concatenate([jnp.where(side, first, swapped(second)), jnp.where(side, swapped(first), second)], 0)


def rows_kernel(full, ids_ref, table_ref, out_ref):
    nodes = out_ref.shape[0]
    per_owner = ids_ref.shape[1]
    rest = per_owner - full * LANES
    height, rows = table_ref.shape
    lines = [ids_ref[n : n + 1, :] for n in range(nodes)]
    ids = [lines[n][:, c * LANES : (c + 1) * LANES] for c in range(full) for n in range(nodes)]
    if rest:
        last = [line[:, full * LANES :] for line in lines]
        if rest < HALF:
            last = [jnp.concatenate([x, jnp.full((1, HALF - rest), -1, jnp.int32)], 1) for x in last]
        ids += [jnp.concatenate(last[n : n + 2], 1) for n in range(0, nodes, 2)]
    ids = jnp.concatenate(ids, 1)
    picked = mm(table_ref[...], hot(iota((rows, ids.shape[1]), 0) == ids))
    for c in range(full):
        for n in range(nodes):
            at = (c * nodes + n) * LANES
            out_ref[n, c * height : (c + 1) * height, :] = picked[:, at : at + LANES].astype(bf16)
    if rest:
        room = out_ref.shape[1] - full * height
        for n in range(0, nodes, 2):
            at = full * nodes * LANES + n * HALF
            for i, piece in enumerate(split_pair(picked[:, at : at + LANES])):
                if room > height // 2:
                    piece = jnp.concatenate([piece, jnp.zeros((room - height // 2, LANES), f32)], 0)
                out_ref[n + i, full * height :, :] = piece.astype(bf16)


def message_kernel(mem, per_owner, full, feat, own, feat_ref, rows_ref, slot_ref, time_ref, freq_ref, phase_ref, *rest_refs):
    pack_refs = rest_refs[:feat]
    table_out, out_ref, table_ref, w_ref, edge_ref, sem = rest_refs[feat:]
    nodes = rows_ref.shape[0]
    slots = table_ref.shape[1]
    events = slot_ref.shape[1]
    time = freq_ref.shape[0]
    rest = per_owner - full * LANES
    height = rounded(mem + 2, 16)
    source_of = [lax.rem(feat_ref[0] + feat - k, feat) for k in range(feat)]
    table_ref[height:, :] = jnp.zeros((table_ref.shape[0] - height, slots), bf16)
    for c in range(full):
        for n in range(nodes):
            at = (c * nodes + n) * LANES
            table_ref[0:height, at : at + LANES] = rows_ref[n, c * height : (c + 1) * height, :]
    if rest:
        for n in range(0, nodes, 2):
            at = full * nodes * LANES + n * HALF
            pair = [rows_ref[n + i, full * height :, :].astype(f32)[: height // 2] for i in range(2)]
            table_ref[0:height, at : at + LANES] = join_pair(*pair).astype(bf16)
    keep = pltpu.make_async_copy(table_ref, table_out, sem)
    keep.start()
    edge_rows = own * events // LANES
    tall = LANES + SPARE_ROWS
    for c in range(PIECES):
        spare = []
        for k in range(feat):
            at = edge_rows + c * tall
            w_ref[k * LANES : (k + 1) * LANES, c * LANES : (c + 1) * LANES] = pack_refs[k][at : at + LANES, :]
            spare.append(pack_refs[k][at + LANES : at + tall, :].astype(f32)[0:1])
        spare.append(jnp.zeros((SPARE_ROWS - feat, LANES), f32))
        w_ref[feat * LANES :, c * LANES : (c + 1) * LANES] = jnp.concatenate(spare, 0).astype(bf16)
    for k in range(feat):
        at = pl.multiple_of(source_of[k] * own, own)
        for c in range(events // LANES):
            edge_ref[pl.ds(at, own), c * LANES : (c + 1) * LANES] = pack_refs[k][c * own : (c + 1) * own, :]
    table = table_ref[0:height, :]
    slot_of = iota((slots, events), 0)
    place = places_of(slot_ref[0:2, :], nodes, per_owner)
    hots = [hot(slot_of == place[i : i + 1, :]) for i in range(2)]
    found = [mm(table, h) for h in hots]
    freq = freq_ref[...]
    phase = phase_ref[...]
    by_edge = mm(w_ref[:, EDGE_AT:COLS], edge_ref[...])
    height_all = w_ref.shape[0]
    ones = iota((height_all, events), 0) == feat * LANES + feat
    sums = None
    for i in range(2):
        stamps = found[i][mem : mem + 1, :] * float(1 << STAMP_SHIFT) + found[i][mem + 1 : mem + 2, :]
        code = cosine(freq * (time_ref[...].astype(f32) - stamps) + phase).astype(bf16)
        sent = mm(w_ref[:, 0:height], found[1 - i].astype(bf16)) + mm(w_ref[:, TIME_AT : TIME_AT + time], code) + by_edge
        part = mm_nt(jnp.where(ones, 1.0, sent).astype(bf16), hots[i])
        sums = part if sums is None else sums + part
    extra = sums[feat * LANES :, :]
    hits = extra[feat : feat + 1, :]
    high = jnp.floor(hits * (1.0 / HIT_BASE))
    low = hits - high * HIT_BASE
    row_id = iota((GROUP, LANES), 0)
    folded = full * LANES + (HALF if rest else 0)
    blank = jnp.zeros((out_ref.shape[1] - folded - GROUP * (full + (1 if rest else 0)), LANES), f32)

    def tail(k, at):
        cut = slice(at, at + LANES)
        return jnp.where(
            row_id == 0, extra[k : k + 1, cut], jnp.where(row_id == 1, high[:, cut], jnp.where(row_id == 2, low[:, cut], 0.0))
        )

    for k in range(feat):
        block = sums[k * LANES : (k + 1) * LANES, :]
        for n in range(0, nodes, 2):
            tails = [[], []]
            for c in range(full):
                for i in range(2):
                    at = (c * nodes + n + i) * LANES
                    out_ref[(n + i) * feat + source_of[k], c * LANES : (c + 1) * LANES, :] = block[:, at : at + LANES].astype(bf16)
                    tails[i].append(tail(k, at))
            if rest:
                at = full * nodes * LANES + n * HALF
                ends = tail(k, at)
                for i, piece in enumerate(split_pair(block[:, at : at + LANES])):
                    out_ref[(n + i) * feat + source_of[k], full * LANES : full * LANES + HALF, :] = piece.astype(bf16)
                    tails[i].append(swapped(ends) if i else ends)
            for i in range(2):
                pieces = tails[i] + ([blank] if blank.shape[0] else [])
                out_ref[(n + i) * feat + source_of[k], folded:, :] = jnp.concatenate(pieces, 0).astype(bf16)
    keep.wait()


def embed_kernel(mem, nodes, per_owner, table_ref, ref_ref, gap_ref, freq_ref, phase_ref, wq_ref, wk_ref, wv_ref, wm_ref, bm_ref, wo_ref, bo_ref, out_ref, hot_ref, key_ref, prod_ref):
    tile, columns = ref_ref.shape
    nbrs = columns - 2
    slots = table_ref.shape[1]
    att = wq_ref.shape[0]
    head = att // HEADS
    slot_of = iota((tile, slots), 1)
    place = places_of(ref_ref[...], nodes, per_owner)
    hot_ref[0:tile, :] = hot(place[:, 0:1] == slot_of)
    for k in range(nbrs):
        hot_ref[(k + 1) * tile : (k + 2) * tile, :] = hot(place[:, 2 + k : 3 + k] == slot_of)
    fetched = mm_nt(hot_ref[...], table_ref[...])
    freq = freq_ref[...]
    phase = phase_ref[...]
    kept = iota((tile, LANES), 1) < mem - LANES
    for k in range(nbrs + 1):
        at = k * tile
        if k == 0:
            angle = jnp.broadcast_to(phase, (tile, 2 * LANES))
        else:
            angle = gap_ref[:, k - 1 : k].astype(f32) * freq + phase
        wave = cosine(angle)
        key_ref[at : at + tile, 0:LANES] = fetched[at : at + tile, :LANES].astype(bf16)
        key_ref[at : at + tile, LANES : 2 * LANES] = jnp.where(kept, fetched[at : at + tile, LANES:], wave[:, :LANES]).astype(bf16)
        key_ref[at : at + tile, 2 * LANES : att] = wave[:, LANES : att - LANES].astype(bf16)
    query = mm(key_ref[0:tile, :], wq_ref[...]) * (1.0 / math.sqrt(head))
    keys = mm(key_ref[tile:, :], wk_ref[...])
    values = mm(key_ref[tile:, :], wv_ref[...])
    for k in range(nbrs):
        prod_ref[k * tile : (k + 1) * tile, :] = keys[k * tile : (k + 1) * tile, :] * query
    prod = prod_ref[...]
    gather = hot((iota((att, LANES), 0) >= head).astype(jnp.int32) == (iota((att, LANES), 1) & 1))
    high = prod.astype(bf16)
    scores = mm(high, gather) + mm((prod - high.astype(f32)).astype(bf16), gather)
    parts = [scores[k * tile : (k + 1) * tile, :] for k in range(nbrs)]
    top = functools.reduce(jnp.maximum, parts)
    parts = [jnp.exp(s - top) for s in parts]
    scale = 1.0 / functools.reduce(jnp.add, parts)
    spread = hot(
        ((iota((LANES, att), 1) >= head).astype(jnp.int32) == (iota((LANES, att), 0) & 1)) & (iota((LANES, att), 0) < 4)
    )
    upper = iota((tile, LANES), 1) < 2
    attended = jnp.zeros((tile, att), f32)
    for k in range(nbrs):
        w = parts[k] * scale
        w_high = w.astype(bf16).astype(f32)
        w = jnp.where(upper, w_high, w - w_high).astype(bf16)
        attended = attended + mm(w, spread) * values[k * tile : (k + 1) * tile, :]
    merged = mm(attended.astype(bf16), wm_ref[0:att, :]) + mm(key_ref[0:tile, 0:mem], wm_ref[att : att + mem, :])
    hidden = jnp.maximum(merged + bm_ref[...], 0.0).astype(bf16)
    out_ref[...] = (mm(hidden, wo_ref[...]) + bo_ref[...]).astype(bf16)


def state_kernel(memory_ref, w_in_ref, w_hid_ref, bias_ref, out_ref):
    memory = memory_ref[...]
    mem = memory.shape[0]
    bias = bias_ref[...]

    def part(w, g):
        out_ref[g] = jnp.dot(w, memory, precision=exact, preferred_element_type=f32) + bias[:, g : g + 1]

    part(w_in_ref[0, :, 0:mem] + w_hid_ref[0], 0)
    part(w_in_ref[1, :, 0:mem] + w_hid_ref[1], 1)
    part(w_in_ref[2, :, 0:mem], 2)
    part(w_hid_ref[2], 3)


def update_kernel(full, rest, feat, feat_ref, recv_ref, ids_ref, state_hbm, own_hbm, out_ref, acc_ref, state_ref, own_ref, sem):
    rows = acc_ref.shape[1]
    width = own_ref.shape[0]
    loads = [pltpu.make_async_copy(state_hbm, state_ref, sem.at[0]), pltpu.make_async_copy(own_hbm, own_ref, sem.at[1])]
    for load in loads:
        load.start()
    acc_ref[...] = jnp.zeros_like(acc_ref)
    folded = full * LANES + (HALF if rest else 0)
    source_of = [lax.rem(feat_ref[0] + feat - k, feat) for k in range(feat)]

    def step(i, carry):
        main, side = [], []
        tails = [recv_ref[i * feat + source_of[b], folded:, :].astype(f32) for b in range(feat)]
        for c in range(full):
            for b in range(feat):
                main.append(recv_ref[i * feat + source_of[b], c * LANES : (c + 1) * LANES, :])
                side.append(tails[b][c * GROUP : (c + 1) * GROUP])
        if rest:
            for b in range(0, feat, 2):
                pair = [recv_ref[i * feat + source_of[b + j], full * LANES : folded, :].astype(f32) for j in range(2)]
                main.append(join_pair(*pair).astype(bf16))
                ends = [tails[b + j][full * GROUP : (full + 1) * GROUP] for j in range(2)]
                side.append(jnp.where(left(ends[0].shape), ends[0], swapped(ends[1])))
        side = jnp.concatenate(side, 1)
        side = jnp.concatenate([side, jnp.zeros((16 - GROUP, side.shape[1]), f32)], 0).astype(bf16)
        data = jnp.concatenate([jnp.concatenate(main, 1), side], 0)
        ids = ids_ref[i]
        data = jnp.concatenate([data * hot((ids >= h * rows) & (ids < (h + 1) * rows)) for h in range(SPLIT)], 0)
        acc_ref[...] += mm_nt(data, hot(iota((rows, ids.shape[1]), 0) == ids % rows))
        return carry

    steps = recv_ref.shape[0] // feat
    lax.fori_loop(0, steps, step, 0, unroll=steps <= 8)
    for load in loads:
        load.wait()
    height = acc_ref.shape[0] // SPLIT
    acc = jnp.concatenate([acc_ref[h * height : (h + 1) * height, :] for h in range(SPLIT)], 1)
    at = 3 * width
    hits = acc[at : at + 1, :] * HIT_BASE + acc[at + 1 : at + 2, :]
    scale = 1.0 / jnp.maximum(hits, 1.0)
    own = own_ref[...]
    reset = jax.nn.sigmoid(acc[0:width, :] * scale + state_ref[0])
    update = jax.nn.sigmoid(acc[width : 2 * width, :] * scale + state_ref[1])
    fresh = jnp.tanh(acc[2 * width : 3 * width, :] * scale + state_ref[2] + reset * state_ref[3])
    out_ref[...] = jnp.where(hits > 0.0, (1.0 - update) * fresh + update * own, own)


def modest():
    return pltpu.CompilerParams(vmem_limit_bytes=40 << 20)


def on_chip(shape, kind):
    return pltpu.VMEM(shape, kind)


def hold(x):
    return pltpu.with_memory_space_constraint(x, pltpu.VMEM)


def off_chip(x):
    return pltpu.with_memory_space_constraint(x, pltpu.HBM)


def cost(flops, moved):
    return pl.CostEstimate(flops=int(flops), transcendentals=0, bytes_accessed=int(moved))


def per_device(
    memory,
    last_update,
    ev_time,
    nbr_gap,
    slot_rows,
    slot_ref,
    edge_feat,
    frequency,
    phase_shift,
    w_query,
    w_key,
    w_value,
    w_merge,
    b_merge,
    w_out,
    b_out,
    w_input,
    w_hidden,
    gru_bias,
):
    nodes = lax.axis_size("node")
    feat = lax.axis_size("feat")
    blocks = nodes * feat
    rows, mem = memory.shape
    slots = slot_rows.shape[1]
    per_owner = slots // nodes
    events, columns = slot_ref.shape
    time = frequency.shape[0]
    att = w_query.shape[0]
    emb = w_out.shape[1]
    width = w_hidden.shape[2]
    everyone = ("node", "feat")

    asked = slot_rows.reshape(nodes, 1, per_owner)
    asked = lax.all_to_all(asked, "node", split_axis=0, concat_axis=0, tiled=True).reshape(nodes, per_owner)

    here = lax.axis_index("feat").astype(jnp.int32)
    here_line = here.reshape(1)
    memory_t = memory.T
    w_input_t = jnp.swapaxes(w_input, 1, 2)
    w_hidden_t = jnp.swapaxes(w_hidden, 1, 2)
    smem = pl.BlockSpec(memory_space=pltpu.SMEM)
    vmem = pl.BlockSpec(memory_space=pltpu.VMEM)
    hbm = pl.BlockSpec(memory_space=pltpu.HBM)
    auto = pl.BlockSpec()

    own = edge_feat.shape[1]
    height = own * events // LANES + PIECES * (LANES + SPARE_ROWS)
    high_rows = rounded(mem + 2, 16)
    table, *packed = pl.pallas_call(
        functools.partial(pack_kernel, mem, time, feat),
        in_specs=[smem, auto, auto, auto, auto],
        out_shape=[jax.ShapeDtypeStruct((high_rows, rows), bf16)]
        + [jax.ShapeDtypeStruct((height, LANES), bf16)] * feat,
        cost_estimate=cost(1e8, 1e6),
        compiler_params=modest(),
        name="pack",
    )(here_line, off_chip(edge_feat.T), off_chip(w_input_t), off_chip(memory_t), last_update.reshape(1, rows))
    asked, table, *packed = lax.optimization_barrier((asked, table, *packed))
    turn = lambda k: [(i, (i + k) % feat) for i in range(feat)]
    packed = [packed[0]] + [lax.ppermute(packed[k], "feat", turn(k)) for k in range(1, feat)]

    full = per_owner // LANES
    rest = per_owner - full * LANES
    assert rest <= HALF and nodes % 2 == 0
    room = full * high_rows + (rounded(high_rows // 2, 8) if rest else 0)
    found = pl.pallas_call(
        functools.partial(rows_kernel, full),
        out_shape=on_chip((nodes, room, LANES), bf16),
        in_specs=[vmem, vmem],
        out_specs=vmem,
        cost_estimate=cost(1e9, 2e6),
        compiler_params=modest(),
        name="rows",
    )(asked, table)
    found = lax.all_to_all(found, "node", split_axis=0, concat_axis=0, tiled=True)

    state = pl.pallas_call(
        state_kernel,
        out_shape=pltpu.HBM((4, width, rows), f32),
        cost_estimate=cost(3e9, 3e6),
        compiler_params=modest(),
        name="state",
    )(off_chip(memory_t), off_chip(w_input_t), off_chip(w_hidden_t), gru_bias.T)

    places = nodes * (full * LANES + (HALF if rest else 0))
    freq_line = frequency.reshape(1, time)
    phase_line = phase_shift.reshape(1, time)
    shift = mem - LANES
    spread = ((0, 0), (shift, 2 * LANES - shift - time))
    freq_wide, phase_wide = jnp.pad(freq_line, spread), jnp.pad(phase_line, spread)
    own_cols = lax.dynamic_slice_in_dim(memory_t, here * width, width, 0)
    asked = jnp.stack([asked] + [lax.ppermute(asked, "feat", turn(k)) for k in range(1, feat)], 1)
    ids = [asked[:, :, c * LANES : (c + 1) * LANES].reshape(nodes, 1, feat * LANES) for c in range(full)]
    if rest:
        last = jnp.pad(asked[:, :, full * LANES :], ((0, 0), (0, 0), (0, HALF - rest)), constant_values=-1)
        ids.append(last.reshape(nodes, 1, feat * HALF))
    ids = jnp.concatenate(ids, 2)
    found, freq_wide, phase_wide, own_cols, state, ids = lax.optimization_barrier(
        (found, freq_wide, phase_wide, own_cols, state, ids)
    )
    ends = full + (1 if rest else 0)
    depth = full * LANES + (HALF if rest else 0) + rounded(GROUP * ends, 8)
    fetched, sums = pl.pallas_call(
        functools.partial(message_kernel, mem, per_owner, full, feat, own),
        in_specs=[smem] + [vmem] * (5 + feat),
        out_specs=(hbm, vmem),
        out_shape=(
            pltpu.HBM((2 * LANES, places), bf16),
            on_chip((blocks, depth, LANES), bf16),
        ),
        scratch_shapes=[
            pltpu.VMEM((2 * LANES, places), bf16),
            pltpu.VMEM((feat * LANES + SPARE_ROWS, COLS), bf16),
            pltpu.VMEM((feat * own, events), bf16),
            pltpu.SemaphoreType.DMA,
        ],
        cost_estimate=cost(4e9, 4e6),
        compiler_params=modest(),
        name="messages",
    )(
        here_line,
        hold(found),
        slot_ref.T,
        ev_time.reshape(1, events),
        frequency.reshape(time, 1),
        phase_shift.reshape(time, 1),
        *[hold(x) for x in packed],
    )
    sums = lax.all_to_all(sums, everyone, split_axis=0, concat_axis=0, tiled=True)

    nbrs = columns - 2
    whole = lambda shape: pl.BlockSpec(shape, lambda i: (0,) * len(shape))
    embedding = pl.pallas_call(
        functools.partial(embed_kernel, mem, nodes, per_owner),
        grid=(events // EVENT_TILE,),
        in_specs=[
            whole((2 * LANES, places)),
            pl.BlockSpec((EVENT_TILE, columns), lambda i: (i, 0)),
            pl.BlockSpec((EVENT_TILE, nbrs), lambda i: (i, 0)),
            whole((1, 2 * LANES)),
            whole((1, 2 * LANES)),
            whole((att, att)),
            whole((att, att)),
            whole((att, att)),
            whole((att + mem, emb)),
            whole((1, emb)),
            whole((emb, emb)),
            whole((1, emb)),
        ],
        out_specs=pl.BlockSpec((EVENT_TILE, emb), lambda i: (i, 0)),
        out_shape=jax.ShapeDtypeStruct((events, emb), bf16),
        scratch_shapes=[
            pltpu.VMEM(((nbrs + 1) * EVENT_TILE, places), bf16),
            pltpu.VMEM(((nbrs + 1) * EVENT_TILE, att), bf16),
            pltpu.VMEM((nbrs * EVENT_TILE, att), f32),
        ],
        cost_estimate=cost(2e10, 4e6),
        compiler_params=modest(),
        name="embed",
    )(
        off_chip(fetched),
        slot_ref,
        nbr_gap,
        freq_wide,
        phase_wide,
        off_chip(w_query),
        off_chip(w_key),
        off_chip(w_value),
        w_merge,
        b_merge.reshape(1, emb),
        off_chip(w_out),
        b_out.reshape(1, emb),
    )

    new_memory = pl.pallas_call(
        functools.partial(update_kernel, full, rest, feat),
        in_specs=[smem, vmem, vmem, hbm, hbm],
        out_specs=vmem,
        out_shape=jax.ShapeDtypeStruct((width, rows), f32),
        scratch_shapes=[
            pltpu.VMEM((SPLIT * (LANES + 16), rows // SPLIT), f32),
            pltpu.VMEM((4, width, rows), f32),
            pltpu.VMEM((width, rows), f32),
            pltpu.SemaphoreType.DMA((2,)),
        ],
        cost_estimate=cost(4e9, 4e6),
        compiler_params=modest(),
        name="update",
    )(here_line, hold(sums), ids, off_chip(state), off_chip(own_cols))
    return (embedding, new_memory.T)


def solution(mesh):
    return jax.shard_map(
        per_device,
        mesh=mesh,
        in_specs=(
            P("node", None),
            P("node"),
            P(("node", "feat")),
            P(("node", "feat"), None),
            P(("node", "feat"), None),
            P(("node", "feat"), None),
            P("node", "feat"),
            P(),
            P(),
            P(),
            P(),
            P(),
            P(),
            P(),
            P(),
            P(),
            P(None, None, "feat"),
            P(None, None, "feat"),
            P(None, "feat"),
        ),
        out_specs=(P(("node", "feat"), None), P("node", "feat")),
        check_vma=False,
    )
```

```python
import functools
import math

import jax
import jax.numpy as jnp
from jax import lax
from jax.experimental import pallas as pl
from jax.experimental.pallas import tpu as pltpu
from jax.sharding import PartitionSpec as P


HEADS = 2
LANES = 128
HALF = 64
GROUP = 3
EVENT_TILE = 128
STAMP_SHIFT = 6
HIT_BASE = 32.0
SPLIT = 2

bf16 = jnp.bfloat16
f32 = jnp.float32
exact = lax.Precision.HIGHEST


def rounded(count, step):
    return -(-count // step) * step


def cosine(x):
    turns = jnp.floor(x * (1.0 / math.pi) + 0.5)
    r = x - turns * 3.140625
    r = r - turns * 9.67502593994140625e-4
    r = r - turns * 1.509957990978376432e-7
    half = turns * 0.5
    sign = 1.0 - 4.0 * (half - jnp.floor(half))
    s = r * r
    poly = 1.0 / 479001600.0
    for coef in (-1.0 / 3628800.0, 1.0 / 40320.0, -1.0 / 720.0, 1.0 / 24.0, -0.5, 1.0):
        poly = poly * s + coef
    return poly * sign


def mm(a, b):
    return jnp.dot(a, b, preferred_element_type=f32)


def mm_nt(a, b):
    return lax.dot_general(a, b, (((1,), (1,)), ((), ())), preferred_element_type=f32)


def hot(mask):
    return jnp.where(mask, 1.0, 0.0).astype(bf16)


def iota(shape, axis):
    return lax.broadcasted_iota(jnp.int32, shape, axis)


PART, TIME_AT, EDGE_AT, COLS = 256, 256, 384, 640
PIECES = COLS // LANES
SPARE_ROWS = 16


def pack_kernel(mem, time, feat, feat_ref, edge_ref, w_ref, memory_ref, stamp_ref, table_ref, *out_refs):
    rows = memory_ref.shape[1]
    stamps = stamp_ref[...]
    high = lax.shift_right_logical(stamps, STAMP_SHIFT)
    low = stamps - lax.shift_left(high, STAMP_SHIFT)
    tail = jnp.concatenate([high, low, jnp.zeros((table_ref.shape[0] - mem - 2, rows), jnp.int32)], 0).astype(f32)
    table_ref[...] = jnp.concatenate([memory_ref[...], tail], 0).astype(bf16)
    own, events = edge_ref.shape
    events = events // feat
    gates, width, raw = w_ref.shape
    lines = jnp.concatenate([w_ref[g] for g in range(gates)], 0)
    lines = jnp.concatenate([lines, jnp.zeros((LANES + SPARE_ROWS - gates * width, raw), f32)], 0)
    height = lines.shape[0]
    fill = lambda count: jnp.zeros((height, count), f32)
    lines = jnp.concatenate(
        [
            lines[:, mem : 2 * mem],
            fill(PART - mem),
            lines[:, 2 * mem : 2 * mem + time],
            fill(LANES - time),
            lines[:, 2 * mem + time :],
        ],
        1,
    ).astype(bf16)
    edge_rows = own * events // LANES
    for k, out_ref in enumerate(out_refs):
        dest = lax.rem(feat_ref[0] + k, feat)
        block = edge_ref[:, pl.ds(pl.multiple_of(dest * events, LANES), events)]
        for c in range(events // LANES):
            out_ref[c * own : (c + 1) * own, :] = block[:, c * LANES : (c + 1) * LANES]
        for c in range(PIECES):
            at = edge_rows + c * height
            out_ref[at : at + height, :] = lines[:, c * LANES : (c + 1) * LANES]


def places_of(slot, nodes, per_owner):
    full = per_owner // LANES * LANES
    owner = jnp.zeros_like(slot)
    for n in range(1, nodes):
        owner = owner + (slot >= n * per_owner).astype(jnp.int32)
    within = slot - owner * per_owner
    piece = lax.shift_right_logical(within, 7)
    return jnp.where(
        within < full,
        (piece * nodes + owner) * LANES + within - piece * LANES,
        full * nodes + owner * HALF + within - full,
    )


def swapped(x):
    return pltpu.roll(x, HALF, 1)


def left(shape):
    return iota(shape, 1) < HALF


def split_pair(tile):
    top, low = tile[: tile.shape[0] // 2], tile[tile.shape[0] // 2 :]
    side = left(top.shape)
    return jnp.where(side, top, swapped(low)), jnp.where(side, swapped(top), low)


def join_pair(first, second):
    side = left(first.shape)
    return jnp.concatenate([jnp.where(side, first, swapped(second)), jnp.where(side, swapped(first), second)], 0)


def rows_kernel(full, ids_ref, table_ref, out_ref):
    nodes = out_ref.shape[0]
    per_owner = ids_ref.shape[1]
    rest = per_owner - full * LANES
    height, rows = table_ref.shape
    lines = [ids_ref[n : n + 1, :] for n in range(nodes)]
    ids = [lines[n][:, c * LANES : (c + 1) * LANES] for c in range(full) for n in range(nodes)]
    if rest:
        last = [line[:, full * LANES :] for line in lines]
        if rest < HALF:
            last = [jnp.concatenate([x, jnp.full((1, HALF - rest), -1, jnp.int32)], 1) for x in last]
        ids += [jnp.concatenate(last[n : n + 2], 1) for n in range(0, nodes, 2)]
    ids = jnp.concatenate(ids, 1)
    picked = mm(table_ref[...], hot(iota((rows, ids.shape[1]), 0) == ids))
    for c in range(full):
        for n in range(nodes):
            at = (c * nodes + n) * LANES
            out_ref[n, c * height : (c + 1) * height, :] = picked[:, at : at + LANES].astype(bf16)
    if rest:
        room = out_ref.shape[1] - full * height
        for n in range(0, nodes, 2):
            at = full * nodes * LANES + n * HALF
            for i, piece in enumerate(split_pair(picked[:, at : at + LANES])):
                if room > height // 2:
                    piece = jnp.concatenate([piece, jnp.zeros((room - height // 2, LANES), f32)], 0)
                out_ref[n + i, full * height :, :] = piece.astype(bf16)


def message_kernel(mem, per_owner, full, feat, own, feat_ref, rows_ref, slot_ref, time_ref, freq_ref, phase_ref, *rest_refs):
    pack_refs = rest_refs[:feat]
    table_out, out_ref, table_ref, w_ref, edge_ref, sem = rest_refs[feat:]
    nodes = rows_ref.shape[0]
    slots = table_ref.shape[1]
    events = slot_ref.shape[1]
    time = freq_ref.shape[0]
    rest = per_owner - full * LANES
    height = rounded(mem + 2, 16)
    source_of = [lax.rem(feat_ref[0] + feat - k, feat) for k in range(feat)]
    table_ref[height:, :] = jnp.zeros((table_ref.shape[0] - height, slots), bf16)
    for c in range(full):
        for n in range(nodes):
            at = (c * nodes + n) * LANES
            table_ref[0:height, at : at + LANES] = rows_ref[n, c * height : (c + 1) * height, :]
    if rest:
        for n in range(0, nodes, 2):
            at = full * nodes * LANES + n * HALF
            pair = [rows_ref[n + i, full * height :, :].astype(f32)[: height // 2] for i in range(2)]
            table_ref[0:height, at : at + LANES] = join_pair(*pair).astype(bf16)
    keep = pltpu.make_async_copy(table_ref, table_out, sem)
    keep.start()
    edge_rows = own * events // LANES
    tall = LANES + SPARE_ROWS
    for c in range(PIECES):
        spare = []
        for k in range(feat):
            at = edge_rows + c * tall
            w_ref[k * LANES : (k + 1) * LANES, c * LANES : (c + 1) * LANES] = pack_refs[k][at : at + LANES, :]
            spare.append(pack_refs[k][at + LANES : at + tall, :].astype(f32)[0:1])
        spare.append(jnp.zeros((SPARE_ROWS - feat, LANES), f32))
        w_ref[feat * LANES :, c * LANES : (c + 1) * LANES] = jnp.concatenate(spare, 0).astype(bf16)
    for k in range(feat):
        at = pl.multiple_of(source_of[k] * own, own)
        for c in range(events // LANES):
            edge_ref[pl.ds(at, own), c * LANES : (c + 1) * LANES] = pack_refs[k][c * own : (c + 1) * own, :]
    table = table_ref[0:height, :]
    place = places_of(slot_ref[0:2, :], nodes, per_owner)
    place = jnp.concatenate([place[0:1, :], place[1:2, :]], 1)
    hots = hot(iota((slots, 2 * events), 0) == place)
    both = mm(table, hots)
    found = [both[:, i * events : (i + 1) * events] for i in range(2)]
    freq = freq_ref[...]
    phase = phase_ref[...]
    by_edge = mm(w_ref[:, EDGE_AT:COLS], edge_ref[...])
    height_all = w_ref.shape[0]
    ones = iota((height_all, events), 0) == feat * LANES + feat
    sent = []
    for i in range(2):
        stamps = found[i][mem : mem + 1, :] * float(1 << STAMP_SHIFT) + found[i][mem + 1 : mem + 2, :]
        code = cosine(freq * (time_ref[...].astype(f32) - stamps) + phase).astype(bf16)
        part = mm(w_ref[:, 0:height], found[1 - i].astype(bf16)) + mm(w_ref[:, TIME_AT : TIME_AT + time], code) + by_edge
        sent.append(jnp.where(ones, 1.0, part).astype(bf16))
    sums = mm_nt(jnp.concatenate(sent, 1), hots)
    extra = sums[feat * LANES :, :]
    hits = extra[feat : feat + 1, :]
    high = jnp.floor(hits * (1.0 / HIT_BASE))
    low = hits - high * HIT_BASE
    row_id = iota((GROUP, LANES), 0)
    folded = full * LANES + (HALF if rest else 0)
    blank = jnp.zeros((out_ref.shape[1] - folded - GROUP * (full + (1 if rest else 0)), LANES), f32)

    def tail(k, at):
        cut = slice(at, at + LANES)
        return jnp.where(
            row_id == 0, extra[k : k + 1, cut], jnp.where(row_id == 1, high[:, cut], jnp.where(row_id == 2, low[:, cut], 0.0))
        )

    for k in range(feat):
        block = sums[k * LANES : (k + 1) * LANES, :]
        for n in range(0, nodes, 2):
            tails = [[], []]
            for c in range(full):
                for i in range(2):
                    at = (c * nodes + n + i) * LANES
                    out_ref[(n + i) * feat + source_of[k], c * LANES : (c + 1) * LANES, :] = block[:, at : at + LANES].astype(bf16)
                    tails[i].append(tail(k, at))
            if rest:
                at = full * nodes * LANES + n * HALF
                ends = tail(k, at)
                for i, piece in enumerate(split_pair(block[:, at : at + LANES])):
                    out_ref[(n + i) * feat + source_of[k], full * LANES : full * LANES + HALF, :] = piece.astype(bf16)
                    tails[i].append(swapped(ends) if i else ends)
            for i in range(2):
                pieces = tails[i] + ([blank] if blank.shape[0] else [])
                out_ref[(n + i) * feat + source_of[k], folded:, :] = jnp.concatenate(pieces, 0).astype(bf16)
    keep.wait()


def embed_kernel(mem, nodes, per_owner, table_ref, ref_ref, gap_ref, freq_ref, phase_ref, wq_ref, wk_ref, wv_ref, wm_ref, bm_ref, wo_ref, bo_ref, out_ref, hot_ref, key_ref, prod_ref):
    tile, columns = ref_ref.shape
    nbrs = columns - 2
    slots = table_ref.shape[1]
    att = wq_ref.shape[0]
    head = att // HEADS
    slot_of = iota((tile, slots), 1)
    place = places_of(ref_ref[...], nodes, per_owner)
    hot_ref[0:tile, :] = hot(place[:, 0:1] == slot_of)
    for k in range(nbrs):
        hot_ref[(k + 1) * tile : (k + 2) * tile, :] = hot(place[:, 2 + k : 3 + k] == slot_of)
    fetched = mm_nt(hot_ref[...], table_ref[...])
    freq = freq_ref[...]
    phase = phase_ref[...]
    kept = iota((tile, LANES), 1) < mem - LANES
    for k in range(nbrs + 1):
        at = k * tile
        if k == 0:
            angle = jnp.broadcast_to(phase, (tile, 2 * LANES))
        else:
            angle = gap_ref[:, k - 1 : k].astype(f32) * freq + phase
        wave = cosine(angle)
        key_ref[at : at + tile, 0:LANES] = fetched[at : at + tile, :LANES].astype(bf16)
        key_ref[at : at + tile, LANES : 2 * LANES] = jnp.where(kept, fetched[at : at + tile, LANES:], wave[:, :LANES]).astype(bf16)
        key_ref[at : at + tile, 2 * LANES : att] = wave[:, LANES : att - LANES].astype(bf16)
    query = mm(key_ref[0:tile, :], wq_ref[...]) * (1.0 / math.sqrt(head))
    keys = mm(key_ref[tile:, :], wk_ref[...])
    values = mm(key_ref[tile:, :], wv_ref[...])
    for k in range(nbrs):
        prod_ref[k * tile : (k + 1) * tile, :] = keys[k * tile : (k + 1) * tile, :] * query
    prod = prod_ref[...]
    gather = hot((iota((att, LANES), 0) >= head).astype(jnp.int32) == (iota((att, LANES), 1) & 1))
    high = prod.astype(bf16)
    scores = mm(high, gather) + mm((prod - high.astype(f32)).astype(bf16), gather)
    parts = [scores[k * tile : (k + 1) * tile, :] for k in range(nbrs)]
    top = functools.reduce(jnp.maximum, parts)
    parts = [jnp.exp(s - top) for s in parts]
    scale = 1.0 / functools.reduce(jnp.add, parts)
    spread = hot(
        ((iota((LANES, att), 1) >= head).astype(jnp.int32) == (iota((LANES, att), 0) & 1)) & (iota((LANES, att), 0) < 4)
    )
    upper = iota((tile, LANES), 1) < 2
    attended = jnp.zeros((tile, att), f32)
    for k in range(nbrs):
        w = parts[k] * scale
        w_high = w.astype(bf16).astype(f32)
        w = jnp.where(upper, w_high, w - w_high).astype(bf16)
        attended = attended + mm(w, spread) * values[k * tile : (k + 1) * tile, :]
    merged = mm(attended.astype(bf16), wm_ref[0:att, :]) + mm(key_ref[0:tile, 0:mem], wm_ref[att : att + mem, :])
    hidden = jnp.maximum(merged + bm_ref[...], 0.0).astype(bf16)
    out_ref[...] = (mm(hidden, wo_ref[...]) + bo_ref[...]).astype(bf16)


def state_kernel(memory_ref, w_in_ref, w_hid_ref, bias_ref, out_ref):
    memory = memory_ref[...]
    mem = memory.shape[0]
    bias = bias_ref[...]

    def part(w, g):
        out_ref[g] = jnp.dot(w, memory, precision=exact, preferred_element_type=f32) + bias[:, g : g + 1]

    part(w_in_ref[0, :, 0:mem] + w_hid_ref[0], 0)
    part(w_in_ref[1, :, 0:mem] + w_hid_ref[1], 1)
    part(w_in_ref[2, :, 0:mem], 2)
    part(w_hid_ref[2], 3)


def update_kernel(full, rest, feat, feat_ref, recv_ref, ids_ref, state_hbm, own_hbm, out_ref, acc_ref, state_ref, own_ref, sem):
    rows = acc_ref.shape[1]
    width = own_ref.shape[0]
    loads = [pltpu.make_async_copy(state_hbm, state_ref, sem.at[0]), pltpu.make_async_copy(own_hbm, own_ref, sem.at[1])]
    for load in loads:
        load.start()
    acc_ref[...] = jnp.zeros_like(acc_ref)
    folded = full * LANES + (HALF if rest else 0)
    source_of = [lax.rem(feat_ref[0] + feat - k, feat) for k in range(feat)]

    def step(i, carry):
        main, side = [], []
        tails = [recv_ref[i * feat + source_of[b], folded:, :].astype(f32) for b in range(feat)]
        for c in range(full):
            for b in range(feat):
                main.append(recv_ref[i * feat + source_of[b], c * LANES : (c + 1) * LANES, :])
                side.append(tails[b][c * GROUP : (c + 1) * GROUP])
        if rest:
            for b in range(0, feat, 2):
                pair = [recv_ref[i * feat + source_of[b + j], full * LANES : folded, :].astype(f32) for j in range(2)]
                main.append(join_pair(*pair).astype(bf16))
                ends = [tails[b + j][full * GROUP : (full + 1) * GROUP] for j in range(2)]
                side.append(jnp.where(left(ends[0].shape), ends[0], swapped(ends[1])))
        side = jnp.concatenate(side, 1)
        side = jnp.concatenate([side, jnp.zeros((16 - GROUP, side.shape[1]), f32)], 0).astype(bf16)
        data = jnp.concatenate([jnp.concatenate(main, 1), side], 0)
        ids = ids_ref[i]
        data = jnp.concatenate([data * hot((ids >= h * rows) & (ids < (h + 1) * rows)) for h in range(SPLIT)], 0)
        acc_ref[...] += mm_nt(data, hot(iota((rows, ids.shape[1]), 0) == ids % rows))
        return carry

    steps = recv_ref.shape[0] // feat
    lax.fori_loop(0, steps, step, 0, unroll=steps <= 8)
    for load in loads:
        load.wait()
    height = acc_ref.shape[0] // SPLIT
    acc = jnp.concatenate([acc_ref[h * height : (h + 1) * height, :] for h in range(SPLIT)], 1)
    at = 3 * width
    hits = acc[at : at + 1, :] * HIT_BASE + acc[at + 1 : at + 2, :]
    scale = 1.0 / jnp.maximum(hits, 1.0)
    own = own_ref[...]
    reset = jax.nn.sigmoid(acc[0:width, :] * scale + state_ref[0])
    update = jax.nn.sigmoid(acc[width : 2 * width, :] * scale + state_ref[1])
    fresh = jnp.tanh(acc[2 * width : 3 * width, :] * scale + state_ref[2] + reset * state_ref[3])
    out_ref[...] = jnp.where(hits > 0.0, (1.0 - update) * fresh + update * own, own)


def modest():
    return pltpu.CompilerParams(vmem_limit_bytes=40 << 20)


def on_chip(shape, kind):
    return pltpu.VMEM(shape, kind)


def hold(x):
    return pltpu.with_memory_space_constraint(x, pltpu.VMEM)


def off_chip(x):
    return pltpu.with_memory_space_constraint(x, pltpu.HBM)


def cost(flops, moved):
    return pl.CostEstimate(flops=int(flops), transcendentals=0, bytes_accessed=int(moved))


def per_device(
    memory,
    last_update,
    ev_time,
    nbr_gap,
    slot_rows,
    slot_ref,
    edge_feat,
    frequency,
    phase_shift,
    w_query,
    w_key,
    w_value,
    w_merge,
    b_merge,
    w_out,
    b_out,
    w_input,
    w_hidden,
    gru_bias,
):
    nodes = lax.axis_size("node")
    feat = lax.axis_size("feat")
    blocks = nodes * feat
    rows, mem = memory.shape
    slots = slot_rows.shape[1]
    per_owner = slots // nodes
    events, columns = slot_ref.shape
    time = frequency.shape[0]
    att = w_query.shape[0]
    emb = w_out.shape[1]
    width = w_hidden.shape[2]
    everyone = ("node", "feat")

    asked = slot_rows.reshape(nodes, 1, per_owner)
    asked = lax.all_to_all(asked, "node", split_axis=0, concat_axis=0, tiled=True).reshape(nodes, per_owner)

    here = lax.axis_index("feat").astype(jnp.int32)
    here_line = here.reshape(1)
    memory_t = memory.T
    w_input_t = jnp.swapaxes(w_input, 1, 2)
    w_hidden_t = jnp.swapaxes(w_hidden, 1, 2)
    smem = pl.BlockSpec(memory_space=pltpu.SMEM)
    vmem = pl.BlockSpec(memory_space=pltpu.VMEM)
    hbm = pl.BlockSpec(memory_space=pltpu.HBM)
    auto = pl.BlockSpec()

    own = edge_feat.shape[1]
    height = own * events // LANES + PIECES * (LANES + SPARE_ROWS)
    high_rows = rounded(mem + 2, 16)
    table, *packed = pl.pallas_call(
        functools.partial(pack_kernel, mem, time, feat),
        in_specs=[smem, auto, auto, auto, auto],
        out_shape=[jax.ShapeDtypeStruct((high_rows, rows), bf16)]
        + [jax.ShapeDtypeStruct((height, LANES), bf16)] * feat,
        cost_estimate=cost(1e8, 1e6),
        compiler_params=modest(),
        name="pack",
    )(here_line, off_chip(edge_feat.T), off_chip(w_input_t), off_chip(memory_t), last_update.reshape(1, rows))
    asked, table = lax.optimization_barrier((asked, table))
    turn = lambda k: [(i, (i + k) % feat) for i in range(feat)]
    packed = [packed[0]] + [lax.ppermute(packed[k], "feat", turn(k)) for k in range(1, feat)]

    full = per_owner // LANES
    rest = per_owner - full * LANES
    assert rest <= HALF and nodes % 2 == 0
    room = full * high_rows + (rounded(high_rows // 2, 8) if rest else 0)
    found = pl.pallas_call(
        functools.partial(rows_kernel, full),
        out_shape=on_chip((nodes, room, LANES), bf16),
        in_specs=[vmem, vmem],
        out_specs=vmem,
        cost_estimate=cost(1e9, 2e6),
        compiler_params=modest(),
        name="rows",
    )(asked, table)
    found = lax.all_to_all(found, "node", split_axis=0, concat_axis=0, tiled=True)

    state = pl.pallas_call(
        state_kernel,
        out_shape=pltpu.HBM((4, width, rows), f32),
        cost_estimate=cost(3e9, 3e6),
        compiler_params=modest(),
        name="state",
    )(off_chip(memory_t), off_chip(w_input_t), off_chip(w_hidden_t), gru_bias.T)

    places = nodes * (full * LANES + (HALF if rest else 0))
    freq_line = frequency.reshape(1, time)
    phase_line = phase_shift.reshape(1, time)
    shift = mem - LANES
    spread = ((0, 0), (shift, 2 * LANES - shift - time))
    freq_wide = jnp.pad(freq_line, spread)
    phase_wide = jnp.pad(phase_line, spread)
    own_cols = lax.dynamic_slice_in_dim(memory_t, here * width, width, 0)
    asked = jnp.stack([asked] + [lax.ppermute(asked, "feat", turn(k)) for k in range(1, feat)], 1)
    ids = [asked[:, :, c * LANES : (c + 1) * LANES].reshape(nodes, 1, feat * LANES) for c in range(full)]
    if rest:
        last = jnp.pad(asked[:, :, full * LANES :], ((0, 0), (0, 0), (0, HALF - rest)), constant_values=-1)
        ids.append(last.reshape(nodes, 1, feat * HALF))
    ids = jnp.concatenate(ids, 2)
    found, freq_wide, phase_wide, own_cols, state, ids = lax.optimization_barrier(
        (found, freq_wide, phase_wide, own_cols, state, ids)
    )
    ends = full + (1 if rest else 0)
    depth = full * LANES + (HALF if rest else 0) + rounded(GROUP * ends, 8)
    fetched, sums = pl.pallas_call(
        functools.partial(message_kernel, mem, per_owner, full, feat, own),
        in_specs=[smem] + [vmem] * (5 + feat),
        out_specs=(hbm, vmem),
        out_shape=(
            pltpu.HBM((2 * LANES, places), bf16),
            on_chip((blocks, depth, LANES), bf16),
        ),
        scratch_shapes=[
            pltpu.VMEM((2 * LANES, places), bf16),
            pltpu.VMEM((feat * LANES + SPARE_ROWS, COLS), bf16),
            pltpu.VMEM((feat * own, events), bf16),
            pltpu.SemaphoreType.DMA,
        ],
        cost_estimate=cost(4e9, 4e6),
        compiler_params=modest(),
        name="messages",
    )(
        here_line,
        hold(found),
        slot_ref.T,
        ev_time.reshape(1, events),
        frequency.reshape(time, 1),
        phase_shift.reshape(time, 1),
        *[hold(x) for x in packed],
    )
    sums = lax.all_to_all(sums, everyone, split_axis=0, concat_axis=0, tiled=True)

    nbrs = columns - 2
    whole = lambda shape: pl.BlockSpec(shape, lambda i: (0,) * len(shape))
    embedding = pl.pallas_call(
        functools.partial(embed_kernel, mem, nodes, per_owner),
        grid=(events // EVENT_TILE,),
        in_specs=[
            whole((2 * LANES, places)),
            pl.BlockSpec((EVENT_TILE, columns), lambda i: (i, 0)),
            pl.BlockSpec((EVENT_TILE, nbrs), lambda i: (i, 0)),
            whole((1, 2 * LANES)),
            whole((1, 2 * LANES)),
            whole((att, att)),
            whole((att, att)),
            whole((att, att)),
            whole((att + mem, emb)),
            whole((1, emb)),
            whole((emb, emb)),
            whole((1, emb)),
        ],
        out_specs=pl.BlockSpec((EVENT_TILE, emb), lambda i: (i, 0)),
        out_shape=jax.ShapeDtypeStruct((events, emb), bf16),
        scratch_shapes=[
            pltpu.VMEM(((nbrs + 1) * EVENT_TILE, places), bf16),
            pltpu.VMEM(((nbrs + 1) * EVENT_TILE, att), bf16),
            pltpu.VMEM((nbrs * EVENT_TILE, att), f32),
        ],
        cost_estimate=cost(2e10, 4e6),
        compiler_params=modest(),
        name="embed",
    )(
        off_chip(fetched),
        slot_ref,
        nbr_gap,
        freq_wide,
        phase_wide,
        off_chip(w_query),
        off_chip(w_key),
        off_chip(w_value),
        w_merge,
        b_merge.reshape(1, emb),
        off_chip(w_out),
        b_out.reshape(1, emb),
    )

    new_memory = pl.pallas_call(
        functools.partial(update_kernel, full, rest, feat),
        in_specs=[smem, vmem, vmem, hbm, hbm],
        out_specs=vmem,
        out_shape=jax.ShapeDtypeStruct((width, rows), f32),
        scratch_shapes=[
            pltpu.VMEM((SPLIT * (LANES + 16), rows // SPLIT), f32),
            pltpu.VMEM((4, width, rows), f32),
            pltpu.VMEM((width, rows), f32),
            pltpu.SemaphoreType.DMA((2,)),
        ],
        cost_estimate=cost(4e9, 4e6),
        compiler_params=modest(),
        name="update",
    )(here_line, hold(sums), ids, off_chip(state), off_chip(own_cols))
    return (embedding, new_memory.T)


def solution(mesh):
    return jax.shard_map(
        per_device,
        mesh=mesh,
        in_specs=(
            P("node", None),
            P("node"),
            P(("node", "feat")),
            P(("node", "feat"), None),
            P(("node", "feat"), None),
            P(("node", "feat"), None),
            P("node", "feat"),
            P(),
            P(),
            P(),
            P(),
            P(),
            P(),
            P(),
            P(),
            P(),
            P(None, None, "feat"),
            P(None, None, "feat"),
            P(None, "feat"),
        ),
        out_specs=(P(("node", "feat"), None), P("node", "feat")),
        check_vma=False,
    )
```

```python
import functools
import math

import jax
import jax.numpy as jnp
from jax import lax
from jax.experimental import pallas as pl
from jax.experimental.pallas import tpu as pltpu
from jax.sharding import PartitionSpec as P


HEADS = 2
LANES = 128
HALF = 64
GROUP = 3
EVENT_TILE = 128
STAMP_SHIFT = 6
HIT_BASE = 32.0
SPLIT = 2

bf16 = jnp.bfloat16
f32 = jnp.float32
exact = lax.Precision.HIGHEST


def rounded(count, step):
    return -(-count // step) * step


def cosine(x):
    turns = jnp.floor(x * (1.0 / math.pi) + 0.5)
    r = x - turns * 3.140625
    r = r - turns * 9.67502593994140625e-4
    r = r - turns * 1.509957990978376432e-7
    half = turns * 0.5
    sign = 1.0 - 4.0 * (half - jnp.floor(half))
    s = r * r
    poly = 1.0 / 479001600.0
    for coef in (-1.0 / 3628800.0, 1.0 / 40320.0, -1.0 / 720.0, 1.0 / 24.0, -0.5, 1.0):
        poly = poly * s + coef
    return poly * sign


def mm(a, b):
    return jnp.dot(a, b, preferred_element_type=f32)


def mm_nt(a, b):
    return lax.dot_general(a, b, (((1,), (1,)), ((), ())), preferred_element_type=f32)


def hot(mask):
    return jnp.where(mask, 1.0, 0.0).astype(bf16)


def iota(shape, axis):
    return lax.broadcasted_iota(jnp.int32, shape, axis)


PART, TIME_AT, EDGE_AT, COLS = 256, 256, 384, 640
PIECES = COLS // LANES
SPARE_ROWS = 16


def pack_kernel(mem, time, feat, feat_ref, edge_ref, w_ref, memory_ref, stamp_ref, table_ref, *out_refs):
    rows = memory_ref.shape[1]
    stamps = stamp_ref[...]
    high = lax.shift_right_logical(stamps, STAMP_SHIFT)
    low = stamps - lax.shift_left(high, STAMP_SHIFT)
    tail = jnp.concatenate([high, low, jnp.zeros((table_ref.shape[0] - mem - 2, rows), jnp.int32)], 0).astype(f32)
    table_ref[...] = jnp.concatenate([memory_ref[...], tail], 0).astype(bf16)
    own, events = edge_ref.shape
    events = events // feat
    gates, width, raw = w_ref.shape
    lines = jnp.concatenate([w_ref[g] for g in range(gates)], 0)
    lines = jnp.concatenate([lines, jnp.zeros((LANES + SPARE_ROWS - gates * width, raw), f32)], 0)
    height = lines.shape[0]
    fill = lambda count: jnp.zeros((height, count), f32)
    lines = jnp.concatenate(
        [
            lines[:, mem : 2 * mem],
            fill(PART - mem),
            lines[:, 2 * mem : 2 * mem + time],
            fill(LANES - time),
            lines[:, 2 * mem + time :],
        ],
        1,
    ).astype(bf16)
    edge_rows = own * events // LANES
    for k, out_ref in enumerate(out_refs):
        dest = lax.rem(feat_ref[0] + k, feat)
        block = edge_ref[:, pl.ds(pl.multiple_of(dest * events, LANES), events)]
        for c in range(events // LANES):
            out_ref[c * own : (c + 1) * own, :] = block[:, c * LANES : (c + 1) * LANES]
        for c in range(PIECES):
            at = edge_rows + c * height
            out_ref[at : at + height, :] = lines[:, c * LANES : (c + 1) * LANES]


def places_of(slot, nodes, per_owner):
    full = per_owner // LANES * LANES
    owner = jnp.zeros_like(slot)
    for n in range(1, nodes):
        owner = owner + (slot >= n * per_owner).astype(jnp.int32)
    within = slot - owner * per_owner
    piece = lax.shift_right_logical(within, 7)
    return jnp.where(
        within < full,
        (piece * nodes + owner) * LANES + within - piece * LANES,
        full * nodes + owner * HALF + within - full,
    )


def swapped(x):
    return pltpu.roll(x, HALF, 1)


def left(shape):
    return iota(shape, 1) < HALF


def split_pair(tile):
    top, low = tile[: tile.shape[0] // 2], tile[tile.shape[0] // 2 :]
    side = left(top.shape)
    return jnp.where(side, top, swapped(low)), jnp.where(side, swapped(top), low)


def join_pair(first, second):
    side = left(first.shape)
    return jnp.concatenate([jnp.where(side, first, swapped(second)), jnp.where(side, swapped(first), second)], 0)


def rows_kernel(full, ids_ref, table_ref, out_ref):
    nodes = out_ref.shape[0]
    per_owner = ids_ref.shape[1]
    rest = per_owner - full * LANES
    height, rows = table_ref.shape
    lines = [ids_ref[n : n + 1, :] for n in range(nodes)]
    ids = [lines[n][:, c * LANES : (c + 1) * LANES] for c in range(full) for n in range(nodes)]
    if rest:
        last = [line[:, full * LANES :] for line in lines]
        if rest < HALF:
            last = [jnp.concatenate([x, jnp.full((1, HALF - rest), -1, jnp.int32)], 1) for x in last]
        ids += [jnp.concatenate(last[n : n + 2], 1) for n in range(0, nodes, 2)]
    ids = jnp.concatenate(ids, 1)
    picked = mm(table_ref[...], hot(iota((rows, ids.shape[1]), 0) == ids))
    for c in range(full):
        for n in range(nodes):
            at = (c * nodes + n) * LANES
            out_ref[n, c * height : (c + 1) * height, :] = picked[:, at : at + LANES].astype(bf16)
    if rest:
        room = out_ref.shape[1] - full * height
        for n in range(0, nodes, 2):
            at = full * nodes * LANES + n * HALF
            for i, piece in enumerate(split_pair(picked[:, at : at + LANES])):
                if room > height // 2:
                    piece = jnp.concatenate([piece, jnp.zeros((room - height // 2, LANES), f32)], 0)
                out_ref[n + i, full * height :, :] = piece.astype(bf16)


def message_kernel(mem, per_owner, full, feat, own, feat_ref, rows_ref, slot_ref, time_ref, freq_ref, phase_ref, *rest_refs):
    pack_refs = rest_refs[:feat]
    table_out, out_ref, table_ref, w_ref, edge_ref, sem = rest_refs[feat:]
    nodes = rows_ref.shape[0]
    slots = table_ref.shape[1]
    events = slot_ref.shape[1]
    time = freq_ref.shape[0]
    rest = per_owner - full * LANES
    height = rounded(mem + 2, 16)
    source_of = [lax.rem(feat_ref[0] + feat - k, feat) for k in range(feat)]
    table_ref[height:, :] = jnp.zeros((table_ref.shape[0] - height, slots), bf16)
    for c in range(full):
        for n in range(nodes):
            at = (c * nodes + n) * LANES
            table_ref[0:height, at : at + LANES] = rows_ref[n, c * height : (c + 1) * height, :]
    if rest:
        for n in range(0, nodes, 2):
            at = full * nodes * LANES + n * HALF
            pair = [rows_ref[n + i, full * height :, :].astype(f32)[: height // 2] for i in range(2)]
            table_ref[0:height, at : at + LANES] = join_pair(*pair).astype(bf16)
    keep = pltpu.make_async_copy(table_ref, table_out, sem)
    keep.start()
    edge_rows = own * events // LANES
    tall = LANES + SPARE_ROWS
    for c in range(PIECES):
        spare = []
        for k in range(feat):
            at = edge_rows + c * tall
            w_ref[k * LANES : (k + 1) * LANES, c * LANES : (c + 1) * LANES] = pack_refs[k][at : at + LANES, :]
            spare.append(pack_refs[k][at + LANES : at + tall, :].astype(f32)[0:1])
        spare.append(jnp.zeros((SPARE_ROWS - feat, LANES), f32))
        w_ref[feat * LANES :, c * LANES : (c + 1) * LANES] = jnp.concatenate(spare, 0).astype(bf16)
    for k in range(feat):
        at = pl.multiple_of(source_of[k] * own, own)
        for c in range(events // LANES):
            edge_ref[pl.ds(at, own), c * LANES : (c + 1) * LANES] = pack_refs[k][c * own : (c + 1) * own, :]
    table = table_ref[0:height, :]
    place = places_of(slot_ref[0:2, :], nodes, per_owner)
    place = jnp.concatenate([place[0:1, :], place[1:2, :]], 1)
    hots = hot(iota((slots, 2 * events), 0) == place)
    both = mm(table, hots)
    found = [both[:, i * events : (i + 1) * events] for i in range(2)]
    freq = freq_ref[...]
    phase = phase_ref[...]
    by_edge = mm(w_ref[:, EDGE_AT:COLS], edge_ref[...])
    height_all = w_ref.shape[0]
    ones = iota((height_all, events), 0) == feat * LANES + feat
    sent = []
    for i in range(2):
        stamps = found[i][mem : mem + 1, :] * float(1 << STAMP_SHIFT) + found[i][mem + 1 : mem + 2, :]
        code = cosine(freq * (time_ref[...].astype(f32) - stamps) + phase).astype(bf16)
        part = mm(w_ref[:, 0:height], found[1 - i].astype(bf16)) + mm(w_ref[:, TIME_AT : TIME_AT + time], code) + by_edge
        sent.append(jnp.where(ones, 1.0, part).astype(bf16))
    sums = mm_nt(jnp.concatenate(sent, 1), hots)
    extra = sums[feat * LANES :, :]
    hits = extra[feat : feat + 1, :]
    high = jnp.floor(hits * (1.0 / HIT_BASE))
    low = hits - high * HIT_BASE
    row_id = iota((GROUP, LANES), 0)
    folded = full * LANES + (HALF if rest else 0)
    blank = jnp.zeros((out_ref.shape[1] - folded - GROUP * (full + (1 if rest else 0)), LANES), f32)

    def tail(k, at):
        cut = slice(at, at + LANES)
        return jnp.where(
            row_id == 0, extra[k : k + 1, cut], jnp.where(row_id == 1, high[:, cut], jnp.where(row_id == 2, low[:, cut], 0.0))
        )

    for k in range(feat):
        block = sums[k * LANES : (k + 1) * LANES, :]
        for n in range(0, nodes, 2):
            tails = [[], []]
            for c in range(full):
                for i in range(2):
                    at = (c * nodes + n + i) * LANES
                    out_ref[(n + i) * feat + source_of[k], c * LANES : (c + 1) * LANES, :] = block[:, at : at + LANES].astype(bf16)
                    tails[i].append(tail(k, at))
            if rest:
                at = full * nodes * LANES + n * HALF
                ends = tail(k, at)
                for i, piece in enumerate(split_pair(block[:, at : at + LANES])):
                    out_ref[(n + i) * feat + source_of[k], full * LANES : full * LANES + HALF, :] = piece.astype(bf16)
                    tails[i].append(swapped(ends) if i else ends)
            for i in range(2):
                pieces = tails[i] + ([blank] if blank.shape[0] else [])
                out_ref[(n + i) * feat + source_of[k], folded:, :] = jnp.concatenate(pieces, 0).astype(bf16)
    keep.wait()


def embed_kernel(mem, nodes, per_owner, table_ref, ref_ref, gap_ref, freq_ref, phase_ref, wq_ref, wk_ref, wv_ref, wm_ref, bm_ref, wo_ref, bo_ref, out_ref, hot_ref, key_ref, prod_ref):
    tile, columns = ref_ref.shape
    nbrs = columns - 2
    slots = table_ref.shape[1]
    att = wq_ref.shape[0]
    head = att // HEADS
    slot_of = iota((tile, slots), 1)
    place = places_of(ref_ref[...], nodes, per_owner)
    hot_ref[0:tile, :] = hot(place[:, 0:1] == slot_of)
    for k in range(nbrs):
        hot_ref[(k + 1) * tile : (k + 2) * tile, :] = hot(place[:, 2 + k : 3 + k] == slot_of)
    fetched = mm_nt(hot_ref[...], table_ref[...])
    freq = freq_ref[...]
    phase = phase_ref[...]
    kept = iota((tile, LANES), 1) < mem - LANES
    for k in range(nbrs + 1):
        at = k * tile
        if k == 0:
            angle = jnp.broadcast_to(phase, (tile, 2 * LANES))
        else:
            angle = gap_ref[:, k - 1 : k].astype(f32) * freq + phase
        wave = cosine(angle)
        key_ref[at : at + tile, 0:LANES] = fetched[at : at + tile, :LANES].astype(bf16)
        key_ref[at : at + tile, LANES : 2 * LANES] = jnp.where(kept, fetched[at : at + tile, LANES:], wave[:, :LANES]).astype(bf16)
        key_ref[at : at + tile, 2 * LANES : att] = wave[:, LANES : att - LANES].astype(bf16)
    query = mm(key_ref[0:tile, :], wq_ref[...]) * (1.0 / math.sqrt(head))
    keys = mm(key_ref[tile:, :], wk_ref[...])
    values = mm(key_ref[tile:, :], wv_ref[...])
    for k in range(nbrs):
        prod_ref[k * tile : (k + 1) * tile, :] = keys[k * tile : (k + 1) * tile, :] * query
    prod = prod_ref[...]
    gather = hot((iota((att, LANES), 0) >= head).astype(jnp.int32) == (iota((att, LANES), 1) & 1))
    high = prod.astype(bf16)
    scores = mm(high, gather) + mm((prod - high.astype(f32)).astype(bf16), gather)
    parts = [scores[k * tile : (k + 1) * tile, :] for k in range(nbrs)]
    top = functools.reduce(jnp.maximum, parts)
    parts = [jnp.exp(s - top) for s in parts]
    scale = 1.0 / functools.reduce(jnp.add, parts)
    spread = hot(
        ((iota((LANES, att), 1) >= head).astype(jnp.int32) == (iota((LANES, att), 0) & 1)) & (iota((LANES, att), 0) < 4)
    )
    upper = iota((tile, LANES), 1) < 2
    attended = jnp.zeros((tile, att), f32)
    for k in range(nbrs):
        w = parts[k] * scale
        w_high = w.astype(bf16).astype(f32)
        w = jnp.where(upper, w_high, w - w_high).astype(bf16)
        attended = attended + mm(w, spread) * values[k * tile : (k + 1) * tile, :]
    merged = mm(attended.astype(bf16), wm_ref[0:att, :]) + mm(key_ref[0:tile, 0:mem], wm_ref[att : att + mem, :])
    hidden = jnp.maximum(merged + bm_ref[...], 0.0).astype(bf16)
    out_ref[...] = (mm(hidden, wo_ref[...]) + bo_ref[...]).astype(bf16)


def state_kernel(memory_ref, w_in_ref, w_hid_ref, bias_ref, out_ref):
    memory = memory_ref[...]
    mem = memory.shape[0]
    bias = bias_ref[...]

    def part(w, g):
        out_ref[g] = jnp.dot(w, memory, precision=exact, preferred_element_type=f32) + bias[:, g : g + 1]

    part(w_in_ref[0, :, 0:mem] + w_hid_ref[0], 0)
    part(w_in_ref[1, :, 0:mem] + w_hid_ref[1], 1)
    part(w_in_ref[2, :, 0:mem], 2)
    part(w_hid_ref[2], 3)


def update_kernel(full, rest, feat, feat_ref, recv_ref, ids_ref, state_hbm, own_hbm, out_ref, acc_ref, state_ref, own_ref, sem):
    rows = acc_ref.shape[1]
    width = own_ref.shape[0]
    loads = [pltpu.make_async_copy(state_hbm, state_ref, sem.at[0]), pltpu.make_async_copy(own_hbm, own_ref, sem.at[1])]
    for load in loads:
        load.start()
    acc_ref[...] = jnp.zeros_like(acc_ref)
    folded = full * LANES + (HALF if rest else 0)
    source_of = [lax.rem(feat_ref[0] + feat - k, feat) for k in range(feat)]

    def step(i, carry):
        main, side = [], []
        tails = [recv_ref[i * feat + source_of[b], folded:, :].astype(f32) for b in range(feat)]
        for c in range(full):
            for b in range(feat):
                main.append(recv_ref[i * feat + source_of[b], c * LANES : (c + 1) * LANES, :])
                side.append(tails[b][c * GROUP : (c + 1) * GROUP])
        if rest:
            for b in range(0, feat, 2):
                pair = [recv_ref[i * feat + source_of[b + j], full * LANES : folded, :].astype(f32) for j in range(2)]
                main.append(join_pair(*pair).astype(bf16))
                ends = [tails[b + j][full * GROUP : (full + 1) * GROUP] for j in range(2)]
                side.append(jnp.where(left(ends[0].shape), ends[0], swapped(ends[1])))
        side = jnp.concatenate(side, 1)
        side = jnp.concatenate([side, jnp.zeros((8 - GROUP, side.shape[1]), f32)], 0)
        main = jnp.concatenate(main, 1)
        ids = ids_ref[i]
        masks = [jnp.where((ids >= h * rows) & (ids < (h + 1) * rows), 1.0, 0.0) for h in range(SPLIT)]
        tails = jnp.concatenate([side * m for m in masks], 0).astype(bf16)
        data = jnp.concatenate([main * m.astype(bf16) for m in masks] + [tails], 0)
        acc_ref[...] += mm_nt(data, hot(iota((rows, ids.shape[1]), 0) == ids % rows))
        return carry

    steps = recv_ref.shape[0] // feat
    lax.fori_loop(0, steps, step, 0, unroll=steps <= 8)
    for load in loads:
        load.wait()
    ends = SPLIT * LANES
    top = jnp.concatenate([acc_ref[h * LANES : (h + 1) * LANES, :] for h in range(SPLIT)], 1)
    low = jnp.concatenate([acc_ref[ends + h * 8 : ends + (h + 1) * 8, :] for h in range(SPLIT)], 1)
    acc = jnp.concatenate([top, low], 0)
    at = 3 * width
    hits = acc[at : at + 1, :] * HIT_BASE + acc[at + 1 : at + 2, :]
    scale = 1.0 / jnp.maximum(hits, 1.0)
    own = own_ref[...]
    reset = jax.nn.sigmoid(acc[0:width, :] * scale + state_ref[0])
    update = jax.nn.sigmoid(acc[width : 2 * width, :] * scale + state_ref[1])
    fresh = jnp.tanh(acc[2 * width : 3 * width, :] * scale + state_ref[2] + reset * state_ref[3])
    out_ref[...] = jnp.where(hits > 0.0, (1.0 - update) * fresh + update * own, own)


def modest():
    return pltpu.CompilerParams(vmem_limit_bytes=40 << 20)


def on_chip(shape, kind):
    return pltpu.VMEM(shape, kind)


def hold(x):
    return pltpu.with_memory_space_constraint(x, pltpu.VMEM)


def off_chip(x):
    return pltpu.with_memory_space_constraint(x, pltpu.HBM)


def cost(flops, moved):
    return pl.CostEstimate(flops=int(flops), transcendentals=0, bytes_accessed=int(moved))


def per_device(
    memory,
    last_update,
    ev_time,
    nbr_gap,
    slot_rows,
    slot_ref,
    edge_feat,
    frequency,
    phase_shift,
    w_query,
    w_key,
    w_value,
    w_merge,
    b_merge,
    w_out,
    b_out,
    w_input,
    w_hidden,
    gru_bias,
):
    nodes = lax.axis_size("node")
    feat = lax.axis_size("feat")
    blocks = nodes * feat
    rows, mem = memory.shape
    slots = slot_rows.shape[1]
    per_owner = slots // nodes
    events, columns = slot_ref.shape
    time = frequency.shape[0]
    att = w_query.shape[0]
    emb = w_out.shape[1]
    width = w_hidden.shape[2]
    everyone = ("node", "feat")

    asked = slot_rows.reshape(nodes, 1, per_owner)
    asked = lax.all_to_all(asked, "node", split_axis=0, concat_axis=0, tiled=True).reshape(nodes, per_owner)

    here = lax.axis_index("feat").astype(jnp.int32)
    here_line = here.reshape(1)
    memory_t = memory.T
    w_input_t = jnp.swapaxes(w_input, 1, 2)
    w_hidden_t = jnp.swapaxes(w_hidden, 1, 2)
    smem = pl.BlockSpec(memory_space=pltpu.SMEM)
    vmem = pl.BlockSpec(memory_space=pltpu.VMEM)
    hbm = pl.BlockSpec(memory_space=pltpu.HBM)
    auto = pl.BlockSpec()

    own = edge_feat.shape[1]
    height = own * events // LANES + PIECES * (LANES + SPARE_ROWS)
    high_rows = rounded(mem + 2, 16)
    table, *packed = pl.pallas_call(
        functools.partial(pack_kernel, mem, time, feat),
        in_specs=[smem, auto, auto, auto, auto],
        out_shape=[jax.ShapeDtypeStruct((high_rows, rows), bf16)]
        + [jax.ShapeDtypeStruct((height, LANES), bf16)] * feat,
        cost_estimate=cost(1e8, 1e6),
        compiler_params=modest(),
        name="pack",
    )(here_line, off_chip(edge_feat.T), off_chip(w_input_t), off_chip(memory_t), last_update.reshape(1, rows))
    asked, table = lax.optimization_barrier((asked, table))
    turn = lambda k: [(i, (i + k) % feat) for i in range(feat)]
    packed = [packed[0]] + [lax.ppermute(packed[k], "feat", turn(k)) for k in range(1, feat)]

    full = per_owner // LANES
    rest = per_owner - full * LANES
    assert rest <= HALF and nodes % 2 == 0
    room = full * high_rows + (rounded(high_rows // 2, 8) if rest else 0)
    found = pl.pallas_call(
        functools.partial(rows_kernel, full),
        out_shape=on_chip((nodes, room, LANES), bf16),
        in_specs=[vmem, vmem],
        out_specs=vmem,
        cost_estimate=cost(1e9, 2e6),
        compiler_params=modest(),
        name="rows",
    )(asked, table)
    found = lax.all_to_all(found, "node", split_axis=0, concat_axis=0, tiled=True)

    state = pl.pallas_call(
        state_kernel,
        out_shape=pltpu.HBM((4, width, rows), f32),
        cost_estimate=cost(3e9, 3e6),
        compiler_params=modest(),
        name="state",
    )(off_chip(memory_t), off_chip(w_input_t), off_chip(w_hidden_t), gru_bias.T)

    places = nodes * (full * LANES + (HALF if rest else 0))
    freq_line = frequency.reshape(1, time)
    phase_line = phase_shift.reshape(1, time)
    shift = mem - LANES
    spread = ((0, 0), (shift, 2 * LANES - shift - time))
    freq_wide = jnp.pad(freq_line, spread)
    phase_wide = jnp.pad(phase_line, spread)
    own_cols = lax.dynamic_slice_in_dim(memory_t, here * width, width, 0)
    asked = jnp.stack([asked] + [lax.ppermute(asked, "feat", turn(k)) for k in range(1, feat)], 1)
    ids = [asked[:, :, c * LANES : (c + 1) * LANES].reshape(nodes, 1, feat * LANES) for c in range(full)]
    if rest:
        last = jnp.pad(asked[:, :, full * LANES :], ((0, 0), (0, 0), (0, HALF - rest)), constant_values=-1)
        ids.append(last.reshape(nodes, 1, feat * HALF))
    ids = jnp.concatenate(ids, 2)
    found, freq_wide, phase_wide, own_cols, state, ids = lax.optimization_barrier(
        (found, freq_wide, phase_wide, own_cols, state, ids)
    )
    ends = full + (1 if rest else 0)
    depth = full * LANES + (HALF if rest else 0) + rounded(GROUP * ends, 8)
    fetched, sums = pl.pallas_call(
        functools.partial(message_kernel, mem, per_owner, full, feat, own),
        in_specs=[smem] + [vmem] * (5 + feat),
        out_specs=(hbm, vmem),
        out_shape=(
            pltpu.HBM((2 * LANES, places), bf16),
            on_chip((blocks, depth, LANES), bf16),
        ),
        scratch_shapes=[
            pltpu.VMEM((2 * LANES, places), bf16),
            pltpu.VMEM((feat * LANES + SPARE_ROWS, COLS), bf16),
            pltpu.VMEM((feat * own, events), bf16),
            pltpu.SemaphoreType.DMA,
        ],
        cost_estimate=cost(4e9, 4e6),
        compiler_params=modest(),
        name="messages",
    )(
        here_line,
        hold(found),
        slot_ref.T,
        ev_time.reshape(1, events),
        frequency.reshape(time, 1),
        phase_shift.reshape(time, 1),
        *[hold(x) for x in packed],
    )
    sums = lax.all_to_all(sums, everyone, split_axis=0, concat_axis=0, tiled=True)

    nbrs = columns - 2
    whole = lambda shape: pl.BlockSpec(shape, lambda i: (0,) * len(shape))
    embedding = pl.pallas_call(
        functools.partial(embed_kernel, mem, nodes, per_owner),
        grid=(events // EVENT_TILE,),
        in_specs=[
            whole((2 * LANES, places)),
            pl.BlockSpec((EVENT_TILE, columns), lambda i: (i, 0)),
            pl.BlockSpec((EVENT_TILE, nbrs), lambda i: (i, 0)),
            whole((1, 2 * LANES)),
            whole((1, 2 * LANES)),
            whole((att, att)),
            whole((att, att)),
            whole((att, att)),
            whole((att + mem, emb)),
            whole((1, emb)),
            whole((emb, emb)),
            whole((1, emb)),
        ],
        out_specs=pl.BlockSpec((EVENT_TILE, emb), lambda i: (i, 0)),
        out_shape=jax.ShapeDtypeStruct((events, emb), bf16),
        scratch_shapes=[
            pltpu.VMEM(((nbrs + 1) * EVENT_TILE, places), bf16),
            pltpu.VMEM(((nbrs + 1) * EVENT_TILE, att), bf16),
            pltpu.VMEM((nbrs * EVENT_TILE, att), f32),
        ],
        cost_estimate=cost(2e10, 4e6),
        compiler_params=modest(),
        name="embed",
    )(
        off_chip(fetched),
        slot_ref,
        nbr_gap,
        freq_wide,
        phase_wide,
        off_chip(w_query),
        off_chip(w_key),
        off_chip(w_value),
        w_merge,
        b_merge.reshape(1, emb),
        off_chip(w_out),
        b_out.reshape(1, emb),
    )

    new_memory = pl.pallas_call(
        functools.partial(update_kernel, full, rest, feat),
        in_specs=[smem, vmem, vmem, hbm, hbm],
        out_specs=vmem,
        out_shape=jax.ShapeDtypeStruct((width, rows), f32),
        scratch_shapes=[
            pltpu.VMEM((SPLIT * (LANES + 8), rows // SPLIT), f32),
            pltpu.VMEM((4, width, rows), f32),
            pltpu.VMEM((width, rows), f32),
            pltpu.SemaphoreType.DMA((2,)),
        ],
        cost_estimate=cost(4e9, 4e6),
        compiler_params=modest(),
        name="update",
    )(here_line, hold(sums), ids, off_chip(state), off_chip(own_cols))
    return (embedding, new_memory.T)


def solution(mesh):
    return jax.shard_map(
        per_device,
        mesh=mesh,
        in_specs=(
            P("node", None),
            P("node"),
            P(("node", "feat")),
            P(("node", "feat"), None),
            P(("node", "feat"), None),
            P(("node", "feat"), None),
            P("node", "feat"),
            P(),
            P(),
            P(),
            P(),
            P(),
            P(),
            P(),
            P(),
            P(),
            P(None, None, "feat"),
            P(None, None, "feat"),
            P(None, "feat"),
        ),
        out_specs=(P(("node", "feat"), None), P("node", "feat")),
        check_vma=False,
    )
```
